8 devices in a mesh: dp: 1 (over z), tp: 2 (over y), sp: 4 (over x, core).
Axes of the slice: x: 2, y: 2, z: 1, core: 2. Of those that a mesh axis runs over, the one named last changes fastest.
Arguments:
- hidden: bfloat16 [64, 4096], P('dp')
- norm_scale: bfloat16 [4096], replicated
- w_qkv: bfloat16 [4096, 6144], P(None, 'tp')
- w_out: bfloat16 [4096, 4096], P('tp')
- k_cache: bfloat16 [64, 512, 8, 128], P('dp', 'sp', 'tp')
- v_cache: bfloat16 [64, 512, 8, 128], P('dp', 'sp', 'tp')
- positions: int32 [64], P('dp')
Outputs:
- output 1: bfloat16 [64, 4096], P('dp')
- output 2: bfloat16 [64, 512, 8, 128], P('dp', 'sp', 'tp')
- output 3: bfloat16 [64, 512, 8, 128], P('dp', 'sp', 'tp')
All inputs are finite; a program needn't handle non-finite values.
Results may differ from the reference program's by a relative error of at most 0.00736725.
Values sent between devices are 32-bit elements.
A program may use at most 1 GiB of HBM per device.

```python
import math
import jax
import jax.numpy as jnp
from jax import lax

BATCH = 64
SEQ = 512
D = 4096
HEADS = 32
KV_HEADS = 8
HEAD = 128


def rope_apply(head_vals, positions):
    half_dim = head_vals.shape[-1] // 2
    inv_freq = jnp.exp(jnp.arange(half_dim, dtype=jnp.float32) * (-2.0 * math.log(500000.0) / head_vals.shape[-1]))
    angles = positions.astype(jnp.float32)[:, None] * inv_freq[None, :]
    cos_part = jnp.cos(angles)[:, None, None, :]
    sin_part = jnp.sin(angles)[:, None, None, :]
    first_half = head_vals[..., :half_dim]
    second_half = head_vals[..., half_dim:]
    return jnp.concatenate([first_half * cos_part - second_half * sin_part, second_half * cos_part + first_half * sin_part], axis=-1)


def setup_inputs(seed: int = 0, part: int = 0) -> dict:
    part_keys = jax.random.split(jax.random.fold_in(jax.random.key(seed), part), 5)
    shared_keys = jax.random.split(jax.random.key(seed + 1), 4)
    qkv_width = (HEADS + 2 * KV_HEADS) * HEAD
    hidden = jax.random.normal(part_keys[0], (BATCH, D), jnp.float32)
    norm_scale = 1.0 + 0.5 * jax.random.normal(shared_keys[0], (D,), jnp.float32)
    col_boost = jnp.where(jax.random.randint(shared_keys[1], (qkv_width,), 0, 16) == 0, 10.0, 1.0)
    w_qkv = jax.random.normal(shared_keys[2], (D, qkv_width), jnp.float32) * col_boost * (D ** -0.5)
    w_out = jax.random.normal(shared_keys[3], (HEADS * HEAD, D), jnp.float32) * (2.0 * (HEADS * HEAD) ** -0.5)
    k_cache = 0.5 * jax.random.normal(part_keys[1], (BATCH, SEQ, KV_HEADS, HEAD), jnp.float32)
    coarse = jax.random.normal(part_keys[2], (BATCH, 8, 1, KV_HEADS, HEAD), jnp.float32)
    fine_part = jax.random.normal(part_keys[3], (BATCH, 8, SEQ // 8, KV_HEADS, HEAD), jnp.float32)
    v_cache = (coarse + 0.5 * fine_part).reshape(BATCH, SEQ, KV_HEADS, HEAD)
    positions = jax.random.randint(part_keys[4], (BATCH,), SEQ // 8, SEQ)
    positions = positions.at[0].set(SEQ - 1).at[1].set(SEQ // 8)
    return {
        'hidden': hidden.astype(jnp.bfloat16),
        'norm_scale': norm_scale.astype(jnp.bfloat16),
        'w_qkv': w_qkv.astype(jnp.bfloat16),
        'w_out': w_out.astype(jnp.bfloat16),
        'k_cache': k_cache.astype(jnp.bfloat16),
        'v_cache': v_cache.astype(jnp.bfloat16),
        'positions': positions.astype(jnp.int32),
    }


def reference(hidden, norm_scale, w_qkv, w_out, k_cache, v_cache, positions):
    q_per_kv = HEADS // KV_HEADS
    hidden_f32 = hidden.astype(jnp.float32)
    row_mean = jnp.mean(hidden_f32, axis=-1, keepdims=True)
    centered = hidden_f32 - row_mean
    row_var = jnp.mean(centered * centered, axis=-1, keepdims=True)
    normed = (centered * lax.rsqrt(row_var + 1e-5) * norm_scale.astype(jnp.float32)).astype(jnp.bfloat16)
    qkv_proj = jnp.clip(jnp.dot(normed, w_qkv, preferred_element_type=jnp.float32).astype(jnp.bfloat16), -8.0, 8.0)
    grouped = qkv_proj.reshape(BATCH, KV_HEADS, q_per_kv + 2, HEAD)
    rotated = rope_apply(grouped[:, :, : q_per_kv + 1].astype(jnp.float32), positions).astype(jnp.bfloat16)
    queries = rotated[:, :, :q_per_kv]
    new_row = (jnp.arange(SEQ)[None, :] == positions[:, None])[:, :, None, None]
    k_upd = jnp.where(new_row, rotated[:, :, q_per_kv][:, None], k_cache)
    v_upd = jnp.where(new_row, grouped[:, :, q_per_kv + 1][:, None], v_cache)

    def one_sequence(seq_args):
        q_seq, k_seq, v_seq, p_seq = seq_args
        scores = jnp.einsum('gqd,sgd->gqs', q_seq.astype(jnp.float32), k_seq.astype(jnp.float32)) * (HEAD ** -0.5)
        valid_mask = jnp.arange(SEQ) <= p_seq
        scores = jnp.where(valid_mask[None, None, :], scores, -jnp.inf)
        weights_bf = jax.nn.softmax(scores, axis=-1).astype(jnp.bfloat16)
        return jnp.einsum('gqs,sgd->gqd', weights_bf.astype(jnp.float32), v_seq.astype(jnp.float32))

    attn_out = lax.map(one_sequence, (queries, k_upd, v_upd, positions))
    attn_flat = attn_out.reshape(BATCH, HEADS * HEAD).astype(jnp.bfloat16)
    h_out = (hidden_f32 + jnp.dot(attn_flat, w_out, preferred_element_type=jnp.float32)).astype(jnp.bfloat16)
    return (h_out, k_upd, v_upd)
```

```python
import functools
import math

import jax
import jax.numpy as jnp
from jax import lax
from jax.experimental import pallas as pl
from jax.experimental.pallas import tpu as pltpu
from jax.sharding import PartitionSpec as P

MESH = pl.DeviceIdType.MESH
NEG = -1e30
UNROLL = 4
W_PARTS = 2
CACHE_PARTS = 8
OUT_CHUNKS = 4
LN_EPS = 1e-5


def attention_kernel(pos_ref, h_ref, scale_ref, w_ref, kc_ref, vc_ref,
                     ko_ref, vo_ref, o_ref, ml_ref,
                     k_ref, v_ref, w_buf, u_ref, q_ref, kn_ref, vn_ref, ang_ref, idx_ref,
                     w_sem, k_sem, v_sem, ko_sem, vo_sem):
    n_seq, d_model = h_ref.shape
    rows = k_ref.shape[1]
    head = k_ref.shape[2]
    kv_local = w_ref.shape[1] // (6 * head)
    group_cols = 6 * head
    base = lax.axis_index('sp') * (rows // kv_local)

    w_rows = d_model // W_PARTS
    c_rows = n_seq // CACHE_PARTS

    def w_copy(g, part):
        at = pl.ds(part * w_rows, w_rows)
        return pltpu.make_async_copy(
            w_ref.at[at, pl.ds(g * group_cols, group_cols)], w_buf.at[g, at], w_sem.at[g, part])

    def c_copies(i):
        at = pl.ds(i * c_rows, c_rows)
        return (pltpu.make_async_copy(kc_ref.at[at], k_ref.at[at], k_sem.at[i]),
                pltpu.make_async_copy(vc_ref.at[at], v_ref.at[at], v_sem.at[i]))

    def out_copies(i):
        at = pl.ds(i * c_rows, c_rows)
        return (pltpu.make_async_copy(k_ref.at[at], ko_ref.at[at], ko_sem.at[i]),
                pltpu.make_async_copy(v_ref.at[at], vo_ref.at[at], vo_sem.at[i]))

    for g in range(kv_local):
        for part in range(W_PARTS):
            w_copy(g, part).start()

    blocks = d_model // 128
    total = jnp.zeros((n_seq, 128), jnp.float32)
    for i in range(blocks):
        total += h_ref[:, i * 128:(i + 1) * 128].astype(jnp.float32)
    mean = jnp.sum(total, axis=1, keepdims=True) * (1.0 / d_model)
    total = jnp.zeros((n_seq, 128), jnp.float32)
    for i in range(blocks):
        cen = h_ref[:, i * 128:(i + 1) * 128].astype(jnp.float32) - mean
        total += cen * cen
    var = jnp.sum(total, axis=1, keepdims=True) * (1.0 / d_model)
    rstd = lax.rsqrt(var + LN_EPS)
    for i in range(blocks):
        cen = h_ref[:, i * 128:(i + 1) * 128].astype(jnp.float32) - mean
        u_ref[:, i * 128:(i + 1) * 128] = (
            cen * rstd * scale_ref[i:i + 1, :].astype(jnp.float32)).astype(jnp.bfloat16)

    lane = lax.broadcasted_iota(jnp.int32, (1, head), 1)
    half = head // 2
    inv_freq = jnp.exp((lane % half).astype(jnp.float32) * (-2.0 * math.log(500000.0) / head))

    def fill(b, _):
        ang_ref[pl.ds(b, 1), :] = jnp.full((1, head), pos_ref[b].astype(jnp.float32)) * inv_freq
        return 0
    lax.fori_loop(0, n_seq, fill, 0)
    cos = jnp.cos(ang_ref[...])
    sin = jnp.sin(ang_ref[...]) * jnp.where(lane < half, -1.0, 1.0)

    def rope(x):
        return (x * cos + pltpu.roll(x, half, 1) * sin).astype(jnp.bfloat16).astype(jnp.float32)

    n_q = 4 * kv_local
    col = lax.broadcasted_iota(jnp.int32, (n_q, rows), 1)
    qg = lax.broadcasted_iota(jnp.int32, (n_q, rows), 0) // 4
    idx_ref[...] = jnp.where(col % kv_local == qg, col // kv_local, 1 << 20)

    started = 0
    for g in range(kv_local):
        acc = jnp.zeros((n_seq, group_cols), jnp.float32)
        for part in range(W_PARTS):
            w_copy(g, part).wait()
            if started < CACHE_PARTS:
                for c in c_copies(started):
                    c.start()
                started += 1
            at = pl.ds(part * w_rows, w_rows)
            acc += jnp.dot(u_ref[:, at], w_buf[g, at, :], preferred_element_type=jnp.float32)
        qkv = jnp.clip(acc.astype(jnp.bfloat16).astype(jnp.float32), -8.0, 8.0)
        for j in range(4):
            q_ref[:, g * 4 + j, :] = rope(qkv[:, j * head:(j + 1) * head])
        kn = rope(qkv[:, 4 * head:5 * head])
        vn = qkv[:, 5 * head:]
        for r in range(16 // kv_local):
            kn_ref[:, r * kv_local + g, :] = kn
            vn_ref[:, r * kv_local + g, :] = vn
    for i in range(started, CACHE_PARTS):
        for c in c_copies(i):
            c.start()

    scale = head ** -0.5
    per = 16 // kv_local
    row16 = lax.broadcasted_iota(jnp.int32, (16, head), 0) // kv_local
    lane_id = lax.broadcasted_iota(jnp.int32, (n_q, 128), 1)

    def insert(b):
        p = pos_ref[b] - base

        @pl.when((p >= 0) & (p < rows // kv_local))
        def _():
            at = pl.ds(pl.multiple_of((p // per) * 16, 16), 16)
            hit = row16 == p % per
            k_ref[b, at, :] = jnp.where(hit, kn_ref[b], k_ref[b, at, :].astype(jnp.float32)).astype(jnp.bfloat16)
            v_ref[b, at, :] = jnp.where(hit, vn_ref[b], v_ref[b, at, :].astype(jnp.float32)).astype(jnp.bfloat16)

    def attend(b, m_all, l_all):
        p = pos_ref[b] - base
        s = lax.dot_general(q_ref[b].astype(jnp.bfloat16), k_ref[b], (((1,), (1,)), ((), ())),
                            preferred_element_type=jnp.float32)
        s = jnp.where(idx_ref[...] <= p, s * scale, NEG)
        m = jnp.max(s, axis=1, keepdims=True)
        e = jnp.exp(s - m)
        l = jnp.sum(e, axis=1, keepdims=True)
        o_ref[b] = jnp.dot(e.astype(jnp.bfloat16), v_ref[b], preferred_element_type=jnp.float32)
        return jnp.where(lane_id == b, m, m_all), jnp.where(lane_id == b, l, l_all)

    m_all = jnp.zeros((n_q, 128), jnp.float32)
    l_all = jnp.zeros((n_q, 128), jnp.float32)
    for i in range(CACHE_PARTS):
        for c in c_copies(i):
            c.wait()

        def step(t, carry):
            b0 = i * c_rows + t * UNROLL
            for k in range(UNROLL):
                insert(b0 + k)
            for k in range(UNROLL):
                carry = attend(b0 + k, *carry)
            return carry
        m_all, l_all = lax.fori_loop(0, c_rows // UNROLL, step, (m_all, l_all))
        for c in out_copies(i):
            c.start()
    ml_ref[0:n_q, :] = m_all
    ml_ref[n_q:, :] = l_all
    for i in range(CACHE_PARTS):
        for c in out_copies(i):
            c.wait()


def finish_kernel(h_ref, w_ref, o_ref, ml_ref, out_ref,
                  w_buf, sib_o, mine_o, sib_ml, send_o, send_ml, x_o, x_ml, att, att_send, lhs,
                  part, y_in, fin, x_in, d_in, d_in2,
                  w_sem, s_sem, r_sem, ys_sem, yr_sem, xs_sem, xr_sem, ds_sem, dr_sem, es_sem, er_sem):
    n_q = ml_ref.shape[0] // 2
    sp = lax.axis_index('sp')
    tp = lax.axis_index('tp')
    x, c = sp // 2, sp % 2
    sib = {'sp': x * 2 + (1 - c)}
    xn = {'sp': (1 - x) * 2 + c}
    yn = {'tp': 1 - tp}

    half_cols = w_buf.shape[1]
    cc = half_cols // OUT_CHUNKS
    q4 = sib_o.shape[0]
    own_col = c * half_cols
    oth_col = (1 - c) * half_cols

    def w_copy(j):
        return pltpu.make_async_copy(
            w_ref.at[:, pl.ds(pl.multiple_of(own_col + j * cc, 128), cc)],
            w_buf.at[:, pl.ds(j * cc, cc)], w_sem.at[j])

    for j in range(OUT_CHUNKS):
        w_copy(j).start()

    barrier = pltpu.get_barrier_semaphore()
    for dev in (sib, xn, yn):
        pl.semaphore_signal(barrier, inc=1, device_id=dev, device_id_type=MESH)
    pl.semaphore_wait(barrier, 3)

    def remote(src, dst, ssem, rsem, dev):
        return pltpu.make_async_remote_copy(src_ref=src, dst_ref=dst, send_sem=ssem, recv_sem=rsem,
                                            device_id=dev, device_id_type=MESH)

    def quarter(xx, k):
        return pl.ds(xx * (2 * q4) + k * q4, q4)

    c_ml = remote(ml_ref, sib_ml, s_sem.at[0], r_sem.at[0], sib)
    c_sib = remote(o_ref.at[quarter(1 - x, 1 - c)], sib_o, s_sem.at[1], r_sem.at[1], sib)
    c_mine = remote(o_ref.at[quarter(x, 1 - c)], mine_o, s_sem.at[2], r_sem.at[2], sib)
    c_ml.start()
    c_sib.start()
    c_mine.start()

    c_ml.wait_recv()
    m0, l0 = ml_ref[:n_q], ml_ref[n_q:]
    m1, l1 = sib_ml[:n_q], sib_ml[n_q:]
    m = jnp.maximum(m0, m1)
    f0, f1 = jnp.exp(m0 - m), jnp.exp(m1 - m)
    l = l0 * f0 + l1 * f1
    send_ml[:n_q] = m
    send_ml[n_q:] = l
    c_xml = remote(send_ml, x_ml, s_sem.at[3], r_sem.at[3], xn)
    c_xml.start()

    def column(a, xx, k, i):
        v = None
        for dx in range(2):
            for dk in range(2):
                at = dx * 2 * q4 + dk * q4 + i
                piece = jnp.broadcast_to(a[:, at:at + 1], (n_q, 128))
                pick = (xx == dx) & (k == dk)
                v = piece if v is None else jnp.where(pick, piece, v)
        return v

    c_sib.wait_recv()
    for i in range(q4):
        at = (1 - x) * (2 * q4) + c * q4 + i
        send_o[i] = (o_ref[at] * column(f0, 1 - x, c, i) + sib_o[i] * column(f1, 1 - x, c, i))
    c_xo = remote(send_o, x_o, s_sem.at[4], r_sem.at[4], xn)
    c_xo.start()

    c_xml.wait_recv()
    m2, l2 = x_ml[:n_q], x_ml[n_q:]
    mm = jnp.maximum(m, m2)
    g, g2 = jnp.exp(m - mm), jnp.exp(m2 - mm)
    inv = 1.0 / (l * g + l2 * g2)
    f0, f1, g2 = f0 * g * inv, f1 * g * inv, g2 * inv
    c_mine.wait_recv()
    for i in range(q4):
        at = x * (2 * q4) + c * q4 + i
        mine_o[i] = o_ref[at] * column(f0, x, c, i) + mine_o[i] * column(f1, x, c, i)
    c_xo.wait_recv()
    for i in range(q4):
        att_send[i] = mine_o[i] + x_o[i] * column(g2, x, c, i)
    c_att = remote(att_send, att.at[pl.ds(c * q4, q4)], s_sem.at[5], r_sem.at[5], sib)
    c_att.start()
    for n in range(n_q):
        lhs[pl.ds(c * q4, q4), n * 128:(n + 1) * 128] = att_send[:, n, :].astype(jnp.bfloat16)
    c_att.wait_recv()
    for n in range(n_q):
        lhs[pl.ds((1 - c) * q4, q4), n * 128:(n + 1) * 128] = (
            att[pl.ds((1 - c) * q4, q4), n, :].astype(jnp.bfloat16))

    y_copy, x_copy, d_copy, e_copy = [], [], [], []
    for j in range(OUT_CHUNKS):
        w_copy(j).wait()
        part[j] = jnp.dot(lhs[...], w_buf[:, j * cc:(j + 1) * cc], preferred_element_type=jnp.float32)
        y_copy.append(remote(part.at[j], y_in.at[j], ys_sem.at[j], yr_sem.at[j], yn))
        y_copy[j].start()

    my_rows = pl.ds(pl.multiple_of(x * (2 * q4), 2 * q4), 2 * q4)
    xn_rows = pl.ds(pl.multiple_of((1 - x) * (2 * q4), 2 * q4), 2 * q4)

    def cols(start, j):
        return pl.ds(pl.multiple_of(start + j * cc, 128), cc)

    for j in range(OUT_CHUNKS):
        y_copy[j].wait_recv()
        fin[j] = h_ref[my_rows, cols(own_col, j)].astype(jnp.float32) + (part[j] + y_in[j])
        x_copy.append(remote(fin.at[j], x_in.at[j], xs_sem.at[j], xr_sem.at[j], xn))
        x_copy[j].start()
        d_copy.append(remote(fin.at[j], d_in.at[j], ds_sem.at[j], dr_sem.at[j], sib))
        d_copy[j].start()
        out_ref[my_rows, cols(own_col, j)] = fin[j].astype(jnp.bfloat16)
    for j in range(OUT_CHUNKS):
        x_copy[j].wait_recv()
        e_copy.append(remote(x_in.at[j], d_in2.at[j], es_sem.at[j], er_sem.at[j], sib))
        e_copy[j].start()
        out_ref[xn_rows, cols(own_col, j)] = x_in[j].astype(jnp.bfloat16)
        d_copy[j].wait_recv()
        out_ref[my_rows, cols(oth_col, j)] = d_in[j].astype(jnp.bfloat16)
    for j in range(OUT_CHUNKS):
        e_copy[j].wait_recv()
        out_ref[xn_rows, cols(oth_col, j)] = d_in2[j].astype(jnp.bfloat16)

    for cp in [c_ml, c_sib, c_mine, c_xml, c_xo, c_att] + y_copy + x_copy + d_copy + e_copy:
        cp.wait_send()


def solution(mesh):
    cache_spec = P('dp', 'sp', 'tp', None)

    def local_step(hidden, norm_scale, w_qkv, w_out, k_cache, v_cache, positions):
        n_seq, seq_local, kv_local, head = k_cache.shape
        d_model = hidden.shape[1]
        rows = seq_local * kv_local
        n_q = 4 * kv_local
        vm = pl.BlockSpec(memory_space=pltpu.VMEM)
        anyspace = pl.BlockSpec(memory_space=pltpu.HBM)
        smem = pl.BlockSpec(memory_space=pltpu.SMEM)
        f32, bf16 = jnp.float32, jnp.bfloat16
        k_upd, v_upd, o, ml = pl.pallas_call(
            attention_kernel,
            out_shape=(jax.ShapeDtypeStruct((n_seq, rows, head), bf16),
                       jax.ShapeDtypeStruct((n_seq, rows, head), bf16),
                       pltpu.VMEM((n_seq, n_q, head), f32),
                       pltpu.VMEM((2 * n_q, 128), f32)),
            in_specs=[smem, vm, vm, anyspace, anyspace, anyspace],
            out_specs=(anyspace, anyspace, vm, vm),
            scratch_shapes=[
                pltpu.VMEM((n_seq, rows, head), bf16),
                pltpu.VMEM((n_seq, rows, head), bf16),
                pltpu.VMEM((kv_local, d_model, 6 * head), bf16),
                pltpu.VMEM((n_seq, d_model), bf16),
                pltpu.VMEM((n_seq, n_q, head), f32),
                pltpu.VMEM((n_seq, 16, head), f32),
                pltpu.VMEM((n_seq, 16, head), f32),
                pltpu.VMEM((n_seq, head), f32),
                pltpu.VMEM((n_q, rows), jnp.int32),
                pltpu.SemaphoreType.DMA((kv_local, W_PARTS)),
                pltpu.SemaphoreType.DMA((CACHE_PARTS,)),
                pltpu.SemaphoreType.DMA((CACHE_PARTS,)),
                pltpu.SemaphoreType.DMA((CACHE_PARTS,)),
                pltpu.SemaphoreType.DMA((CACHE_PARTS,)),
            ],
            compiler_params=pltpu.CompilerParams(vmem_limit_bytes=52 * 1024 * 1024),
            name='attention',
        )(positions, hidden, norm_scale.reshape(d_model // 128, 128), w_qkv,
          k_cache.reshape(n_seq, rows, head), v_cache.reshape(n_seq, rows, head))

        q4 = n_seq // 4
        half_cols = d_model // 2
        cc = half_cols // OUT_CHUNKS
        dma = pltpu.SemaphoreType.DMA
        h_out = pl.pallas_call(
            finish_kernel,
            out_shape=jax.ShapeDtypeStruct((n_seq, d_model), bf16),
            in_specs=[vm, anyspace, vm, vm],
            out_specs=vm,
            scratch_shapes=[
                pltpu.VMEM((w_out.shape[0], half_cols), bf16),
                pltpu.VMEM((q4, n_q, head), f32),
                pltpu.VMEM((q4, n_q, head), f32),
                pltpu.VMEM((2 * n_q, 128), f32),
                pltpu.VMEM((q4, n_q, head), f32),
                pltpu.VMEM((2 * n_q, 128), f32),
                pltpu.VMEM((q4, n_q, head), f32),
                pltpu.VMEM((2 * n_q, 128), f32),
                pltpu.VMEM((2 * q4, n_q, head), f32),
                pltpu.VMEM((q4, n_q, head), f32),
                pltpu.VMEM((2 * q4, n_q * head), bf16),
                pltpu.VMEM((OUT_CHUNKS, 2 * q4, cc), f32),
                pltpu.VMEM((OUT_CHUNKS, 2 * q4, cc), f32),
                pltpu.VMEM((OUT_CHUNKS, 2 * q4, cc), f32),
                pltpu.VMEM((OUT_CHUNKS, 2 * q4, cc), f32),
                pltpu.VMEM((OUT_CHUNKS, 2 * q4, cc), f32),
                pltpu.VMEM((OUT_CHUNKS, 2 * q4, cc), f32),
                dma((OUT_CHUNKS,)), dma((6,)), dma((6,)),
                dma((OUT_CHUNKS,)), dma((OUT_CHUNKS,)),
                dma((OUT_CHUNKS,)), dma((OUT_CHUNKS,)),
                dma((OUT_CHUNKS,)), dma((OUT_CHUNKS,)),
                dma((OUT_CHUNKS,)), dma((OUT_CHUNKS,)),
            ],
            compiler_params=pltpu.CompilerParams(
                collective_id=0, has_side_effects=True, vmem_limit_bytes=56 * 1024 * 1024),
            name='finish',
        )(hidden, w_out, o, ml)
        return h_out, k_upd.reshape(k_cache.shape), v_upd.reshape(v_cache.shape)

    return jax.shard_map(
        local_step,
        mesh=mesh,
        in_specs=(P('dp', None), P(None), P(None, 'tp'), P('tp', None), cache_spec, cache_spec, P('dp')),
        out_specs=(P('dp', None), cache_spec, cache_spec),
        check_vma=False,
    )
```

```python
import functools
import math

import jax
import jax.numpy as jnp
from jax import lax
from jax.experimental import pallas as pl
from jax.experimental.pallas import tpu as pltpu
from jax.sharding import PartitionSpec as P

MESH = pl.DeviceIdType.MESH
NEG = -1e30
PV_LAG = 2
W_PARTS = 2
CACHE_PARTS = 8
OUT_CHUNKS = 4
LN_EPS = 1e-5


def attention_kernel(pos_hbm, h_hbm, scale_hbm, w_ref, kc_ref, vc_ref,
                     ko_ref, vo_ref, o_ref, ml_ref,
                     pos_ref, h_ref, scale_ref, k_ref, v_ref, w_buf, u_ref, q_ref, kn_ref, vn_ref,
                     ang_ref, idx_ref, s_ref,
                     in_sem, w_sem, k_sem, v_sem, ko_sem, vo_sem):
    n_seq, d_model = h_ref.shape
    rows = k_ref.shape[1]
    head = k_ref.shape[2]
    kv_local = w_ref.shape[1] // (6 * head)
    group_cols = 6 * head
    base = lax.axis_index('sp') * (rows // kv_local)

    w_rows = d_model // W_PARTS
    c_rows = n_seq // CACHE_PARTS

    small = [pltpu.make_async_copy(h_hbm, h_ref, in_sem.at[0]),
             pltpu.make_async_copy(scale_hbm, scale_ref, in_sem.at[1]),
             pltpu.make_async_copy(pos_hbm, pos_ref, in_sem.at[2])]
    for cp in small:
        cp.start()

    def w_copy(g, part):
        at = pl.ds(part * w_rows, w_rows)
        return pltpu.make_async_copy(
            w_ref.at[at, pl.ds(g * group_cols, group_cols)], w_buf.at[g, at], w_sem.at[g, part])

    def c_copies(i):
        at = pl.ds(i * c_rows, c_rows)
        return (pltpu.make_async_copy(kc_ref.at[at], k_ref.at[at], k_sem.at[i]),
                pltpu.make_async_copy(vc_ref.at[at], v_ref.at[at], v_sem.at[i]))

    def out_copies(i):
        at = pl.ds(i * c_rows, c_rows)
        return (pltpu.make_async_copy(k_ref.at[at], ko_ref.at[at], ko_sem.at[i]),
                pltpu.make_async_copy(v_ref.at[at], vo_ref.at[at], vo_sem.at[i]))

    for g in range(kv_local):
        for part in range(W_PARTS):
            w_copy(g, part).start()
    for i in range(CACHE_PARTS):
        for c in c_copies(i):
            c.start(priority=1)

    n_q = 4 * kv_local
    col = lax.broadcasted_iota(jnp.int32, (n_q, rows), 1)
    qg = lax.broadcasted_iota(jnp.int32, (n_q, rows), 0) // 4
    idx_ref[...] = jnp.where(col % kv_local == qg, col // kv_local, 1 << 20)

    lane = lax.broadcasted_iota(jnp.int32, (1, head), 1)
    half = head // 2
    inv_freq = jnp.exp((lane % half).astype(jnp.float32) * (-2.0 * math.log(500000.0) / head))
    small[2].wait()

    def fill(b, _):
        ang_ref[pl.ds(b, 1), :] = jnp.full((1, head), pos_ref[b].astype(jnp.float32)) * inv_freq
        return 0
    lax.fori_loop(0, n_seq, fill, 0)
    cos = jnp.cos(ang_ref[...])
    sin = jnp.sin(ang_ref[...]) * jnp.where(lane < half, -1.0, 1.0)

    def rope(x):
        return (x * cos + pltpu.roll(x, half, 1) * sin).astype(jnp.bfloat16).astype(jnp.float32)

    small[0].wait()
    small[1].wait()
    blocks = d_model // 128
    total = jnp.zeros((n_seq, 128), jnp.float32)
    for i in range(blocks):
        total += h_ref[:, i * 128:(i + 1) * 128].astype(jnp.float32)
    mean = jnp.sum(total, axis=1, keepdims=True) * (1.0 / d_model)
    total = jnp.zeros((n_seq, 128), jnp.float32)
    for i in range(blocks):
        cen = h_ref[:, i * 128:(i + 1) * 128].astype(jnp.float32) - mean
        total += cen * cen
    var = jnp.sum(total, axis=1, keepdims=True) * (1.0 / d_model)
    rstd = lax.rsqrt(var + LN_EPS)
    for i in range(blocks):
        cen = h_ref[:, i * 128:(i + 1) * 128].astype(jnp.float32) - mean
        u_ref[:, i * 128:(i + 1) * 128] = (
            cen * rstd * scale_ref[i:i + 1, :].astype(jnp.float32)).astype(jnp.bfloat16)

    for g in range(kv_local):
        acc = jnp.zeros((n_seq, group_cols), jnp.float32)
        for part in range(W_PARTS):
            w_copy(g, part).wait()
            at = pl.ds(part * w_rows, w_rows)
            acc += jnp.dot(u_ref[:, at], w_buf[g, at, :], preferred_element_type=jnp.float32)
        qkv = jnp.clip(acc.astype(jnp.bfloat16).astype(jnp.float32), -8.0, 8.0)
        for j in range(4):
            q_ref[:, g * 4 + j, :] = rope(qkv[:, j * head:(j + 1) * head])
        kn = rope(qkv[:, 4 * head:5 * head])
        vn = qkv[:, 5 * head:]
        for r in range(16 // kv_local):
            kn_ref[:, r * kv_local + g, :] = kn
            vn_ref[:, r * kv_local + g, :] = vn

    scale = head ** -0.5
    per = 16 // kv_local
    row16 = lax.broadcasted_iota(jnp.int32, (16, head), 0) // kv_local
    lane_id = lax.broadcasted_iota(jnp.int32, (n_q, 128), 1)
    last = rows // 16 - 1

    def insert(b):
        p = pos_ref[b] - base
        tile = jnp.clip(p // per, 0, last)
        at = pl.ds(pl.multiple_of(tile * 16, 16), 16)
        hit = row16 == p - tile * per
        k_ref[b, at, :] = jnp.where(hit, kn_ref[b], k_ref[b, at, :].astype(jnp.float32)).astype(jnp.bfloat16)
        v_ref[b, at, :] = jnp.where(hit, vn_ref[b], v_ref[b, at, :].astype(jnp.float32)).astype(jnp.bfloat16)

    def scores(b, slot, k):
        s_ref[slot, k] = lax.dot_general(
            q_ref[b].astype(jnp.bfloat16), k_ref[b], (((1,), (1,)), ((), ())),
            preferred_element_type=jnp.float32)

    def arrive(i):
        for c in c_copies(i):
            c.wait()
        for k in range(c_rows):
            insert(i * c_rows + k)
        for c in out_copies(i):
            c.start(priority=1)

    m_all = jnp.zeros((n_q, 128), jnp.float32)
    l_all = jnp.zeros((n_q, 128), jnp.float32)
    arrive(0)
    for k in range(c_rows):
        scores(k, 0, k)
    for i in range(CACHE_PARTS):
        more = i + 1 < CACHE_PARTS
        if more:
            arrive(i + 1)
        weights = [None] * c_rows
        for k in range(c_rows + PV_LAG):
            if k < c_rows:
                b = i * c_rows + k
                if more:
                    scores(b + c_rows, (i + 1) % 2, k)
                s = jnp.where(idx_ref[...] <= pos_ref[b] - base, s_ref[i % 2, k] * scale, NEG)
                m = jnp.max(s, axis=1, keepdims=True)
                e = jnp.exp(s - m)
                l = jnp.sum(e, axis=1, keepdims=True)
                weights[k] = e.astype(jnp.bfloat16)
                m_all = jnp.where(lane_id == b, m, m_all)
                l_all = jnp.where(lane_id == b, l, l_all)
            if k >= PV_LAG:
                b = i * c_rows + k - PV_LAG
                o_ref[b] = jnp.dot(weights[k - PV_LAG], v_ref[b], preferred_element_type=jnp.float32)
    ml_ref[0:n_q, :] = m_all
    ml_ref[n_q:, :] = l_all
    for i in range(CACHE_PARTS):
        for c in out_copies(i):
            c.wait()


def finish_kernel(h_ref, w_ref, o_ref, ml_ref, out_ref,
                  w_buf, sib_o, mine_o, sib_ml, send_o, send_ml, x_o, x_ml, att, att_send, lhs,
                  part, y_in, fin, x_in, d_in, d_in2,
                  w_sem, s_sem, r_sem, ys_sem, yr_sem, xs_sem, xr_sem, ds_sem, dr_sem, es_sem, er_sem):
    n_q = ml_ref.shape[0] // 2
    sp = lax.axis_index('sp')
    tp = lax.axis_index('tp')
    x, c = sp // 2, sp % 2
    sib = {'sp': x * 2 + (1 - c)}
    xn = {'sp': (1 - x) * 2 + c}
    yn = {'tp': 1 - tp}

    half_cols = w_buf.shape[1]
    cc = half_cols // OUT_CHUNKS
    q4 = sib_o.shape[0]
    own_col = c * half_cols
    oth_col = (1 - c) * half_cols

    def w_copy(j):
        return pltpu.make_async_copy(
            w_ref.at[:, pl.ds(pl.multiple_of(own_col + j * cc, 128), cc)],
            w_buf.at[:, pl.ds(j * cc, cc)], w_sem.at[j])

    for j in range(OUT_CHUNKS):
        w_copy(j).start()

    barrier = pltpu.get_barrier_semaphore()
    for dev in (sib, xn, yn):
        pl.semaphore_signal(barrier, inc=1, device_id=dev, device_id_type=MESH)
    pl.semaphore_wait(barrier, 3)

    def remote(src, dst, ssem, rsem, dev):
        return pltpu.make_async_remote_copy(src_ref=src, dst_ref=dst, send_sem=ssem, recv_sem=rsem,
                                            device_id=dev, device_id_type=MESH)

    def quarter(xx, k):
        return pl.ds(xx * (2 * q4) + k * q4, q4)

    c_ml = remote(ml_ref, sib_ml, s_sem.at[0], r_sem.at[0], sib)
    c_sib = remote(o_ref.at[quarter(1 - x, 1 - c)], sib_o, s_sem.at[1], r_sem.at[1], sib)
    c_mine = remote(o_ref.at[quarter(x, 1 - c)], mine_o, s_sem.at[2], r_sem.at[2], sib)
    c_ml.start()
    c_sib.start()
    c_mine.start()

    c_ml.wait_recv()
    m0, l0 = ml_ref[:n_q], ml_ref[n_q:]
    m1, l1 = sib_ml[:n_q], sib_ml[n_q:]
    m = jnp.maximum(m0, m1)
    f0, f1 = jnp.exp(m0 - m), jnp.exp(m1 - m)
    l = l0 * f0 + l1 * f1
    send_ml[:n_q] = m
    send_ml[n_q:] = l
    c_xml = remote(send_ml, x_ml, s_sem.at[3], r_sem.at[3], xn)
    c_xml.start()

    def column(a, xx, k, i):
        v = None
        for dx in range(2):
            for dk in range(2):
                at = dx * 2 * q4 + dk * q4 + i
                piece = jnp.broadcast_to(a[:, at:at + 1], (n_q, 128))
                pick = (xx == dx) & (k == dk)
                v = piece if v is None else jnp.where(pick, piece, v)
        return v

    c_sib.wait_recv()
    for i in range(q4):
        at = (1 - x) * (2 * q4) + c * q4 + i
        send_o[i] = (o_ref[at] * column(f0, 1 - x, c, i) + sib_o[i] * column(f1, 1 - x, c, i))
    c_xo = remote(send_o, x_o, s_sem.at[4], r_sem.at[4], xn)
    c_xo.start()

    c_xml.wait_recv()
    m2, l2 = x_ml[:n_q], x_ml[n_q:]
    mm = jnp.maximum(m, m2)
    g, g2 = jnp.exp(m - mm), jnp.exp(m2 - mm)
    inv = 1.0 / (l * g + l2 * g2)
    f0, f1, g2 = f0 * g * inv, f1 * g * inv, g2 * inv
    c_mine.wait_recv()
    for i in range(q4):
        at = x * (2 * q4) + c * q4 + i
        mine_o[i] = o_ref[at] * column(f0, x, c, i) + mine_o[i] * column(f1, x, c, i)
    c_xo.wait_recv()
    for i in range(q4):
        att_send[i] = mine_o[i] + x_o[i] * column(g2, x, c, i)
    c_att = remote(att_send, att.at[pl.ds(c * q4, q4)], s_sem.at[5], r_sem.at[5], sib)
    c_att.start()
    for n in range(n_q):
        lhs[pl.ds(c * q4, q4), n * 128:(n + 1) * 128] = att_send[:, n, :].astype(jnp.bfloat16)
    c_att.wait_recv()
    for n in range(n_q):
        lhs[pl.ds((1 - c) * q4, q4), n * 128:(n + 1) * 128] = (
            att[pl.ds((1 - c) * q4, q4), n, :].astype(jnp.bfloat16))

    y_copy, x_copy, d_copy, e_copy = [], [], [], []
    for j in range(OUT_CHUNKS):
        w_copy(j).wait()
        part[j] = jnp.dot(lhs[...], w_buf[:, j * cc:(j + 1) * cc], preferred_element_type=jnp.float32)
        y_copy.append(remote(part.at[j], y_in.at[j], ys_sem.at[j], yr_sem.at[j], yn))
        y_copy[j].start()

    my_rows = pl.ds(pl.multiple_of(x * (2 * q4), 2 * q4), 2 * q4)
    xn_rows = pl.ds(pl.multiple_of((1 - x) * (2 * q4), 2 * q4), 2 * q4)

    def cols(start, j):
        return pl.ds(pl.multiple_of(start + j * cc, 128), cc)

    for j in range(OUT_CHUNKS):
        y_copy[j].wait_recv()
        fin[j] = h_ref[my_rows, cols(own_col, j)].astype(jnp.float32) + (part[j] + y_in[j])
        x_copy.append(remote(fin.at[j], x_in.at[j], xs_sem.at[j], xr_sem.at[j], xn))
        x_copy[j].start()
        d_copy.append(remote(fin.at[j], d_in.at[j], ds_sem.at[j], dr_sem.at[j], sib))
        d_copy[j].start()
        out_ref[my_rows, cols(own_col, j)] = fin[j].astype(jnp.bfloat16)
    for j in range(OUT_CHUNKS):
        x_copy[j].wait_recv()
        e_copy.append(remote(x_in.at[j], d_in2.at[j], es_sem.at[j], er_sem.at[j], sib))
        e_copy[j].start()
        out_ref[xn_rows, cols(own_col, j)] = x_in[j].astype(jnp.bfloat16)
        d_copy[j].wait_recv()
        out_ref[my_rows, cols(oth_col, j)] = d_in[j].astype(jnp.bfloat16)
    for j in range(OUT_CHUNKS):
        e_copy[j].wait_recv()
        out_ref[xn_rows, cols(oth_col, j)] = d_in2[j].astype(jnp.bfloat16)

    for cp in [c_ml, c_sib, c_mine, c_xml, c_xo, c_att] + y_copy + x_copy + d_copy + e_copy:
        cp.wait_send()


def solution(mesh):
    cache_spec = P('dp', 'sp', 'tp', None)

    def local_step(hidden, norm_scale, w_qkv, w_out, k_cache, v_cache, positions):
        n_seq, seq_local, kv_local, head = k_cache.shape
        d_model = hidden.shape[1]
        rows = seq_local * kv_local
        n_q = 4 * kv_local
        vm = pl.BlockSpec(memory_space=pltpu.VMEM)
        anyspace = pl.BlockSpec(memory_space=pltpu.HBM)
        f32, bf16 = jnp.float32, jnp.bfloat16
        k_upd, v_upd, o, ml = pl.pallas_call(
            attention_kernel,
            out_shape=(jax.ShapeDtypeStruct((n_seq, rows, head), bf16),
                       jax.ShapeDtypeStruct((n_seq, rows, head), bf16),
                       pltpu.VMEM((n_seq, n_q, head), f32),
                       pltpu.VMEM((2 * n_q, 128), f32)),
            in_specs=[anyspace] * 6,
            out_specs=(anyspace, anyspace, vm, vm),
            scratch_shapes=[
                pltpu.SMEM((n_seq,), jnp.int32),
                pltpu.VMEM((n_seq, d_model), bf16),
                pltpu.VMEM((d_model // 128, 128), bf16),
                pltpu.VMEM((n_seq, rows, head), bf16),
                pltpu.VMEM((n_seq, rows, head), bf16),
                pltpu.VMEM((kv_local, d_model, 6 * head), bf16),
                pltpu.VMEM((n_seq, d_model), bf16),
                pltpu.VMEM((n_seq, n_q, head), f32),
                pltpu.VMEM((n_seq, 16, head), f32),
                pltpu.VMEM((n_seq, 16, head), f32),
                pltpu.VMEM((n_seq, head), f32),
                pltpu.VMEM((n_q, rows), jnp.int32),
                pltpu.VMEM((2, n_seq // CACHE_PARTS, n_q, rows), f32),
                pltpu.SemaphoreType.DMA((3,)),
                pltpu.SemaphoreType.DMA((kv_local, W_PARTS)),
                pltpu.SemaphoreType.DMA((CACHE_PARTS,)),
                pltpu.SemaphoreType.DMA((CACHE_PARTS,)),
                pltpu.SemaphoreType.DMA((CACHE_PARTS,)),
                pltpu.SemaphoreType.DMA((CACHE_PARTS,)),
            ],
            compiler_params=pltpu.CompilerParams(vmem_limit_bytes=54 * 1024 * 1024),
            name='attention',
        )(positions, hidden, norm_scale.reshape(d_model // 128, 128), w_qkv,
          k_cache.reshape(n_seq, rows, head), v_cache.reshape(n_seq, rows, head))

        q4 = n_seq // 4
        half_cols = d_model // 2
        cc = half_cols // OUT_CHUNKS
        dma = pltpu.SemaphoreType.DMA
        h_out = pl.pallas_call(
            finish_kernel,
            out_shape=jax.ShapeDtypeStruct((n_seq, d_model), bf16),
            in_specs=[vm, anyspace, vm, vm],
            out_specs=vm,
            scratch_shapes=[
                pltpu.VMEM((w_out.shape[0], half_cols), bf16),
                pltpu.VMEM((q4, n_q, head), f32),
                pltpu.VMEM((q4, n_q, head), f32),
                pltpu.VMEM((2 * n_q, 128), f32),
                pltpu.VMEM((q4, n_q, head), f32),
                pltpu.VMEM((2 * n_q, 128), f32),
                pltpu.VMEM((q4, n_q, head), f32),
                pltpu.VMEM((2 * n_q, 128), f32),
                pltpu.VMEM((2 * q4, n_q, head), f32),
                pltpu.VMEM((q4, n_q, head), f32),
                pltpu.VMEM((2 * q4, n_q * head), bf16),
                pltpu.VMEM((OUT_CHUNKS, 2 * q4, cc), f32),
                pltpu.VMEM((OUT_CHUNKS, 2 * q4, cc), f32),
                pltpu.VMEM((OUT_CHUNKS, 2 * q4, cc), f32),
                pltpu.VMEM((OUT_CHUNKS, 2 * q4, cc), f32),
                pltpu.VMEM((OUT_CHUNKS, 2 * q4, cc), f32),
                pltpu.VMEM((OUT_CHUNKS, 2 * q4, cc), f32),
                dma((OUT_CHUNKS,)), dma((6,)), dma((6,)),
                dma((OUT_CHUNKS,)), dma((OUT_CHUNKS,)),
                dma((OUT_CHUNKS,)), dma((OUT_CHUNKS,)),
                dma((OUT_CHUNKS,)), dma((OUT_CHUNKS,)),
                dma((OUT_CHUNKS,)), dma((OUT_CHUNKS,)),
            ],
            compiler_params=pltpu.CompilerParams(
                collective_id=0, has_side_effects=True, vmem_limit_bytes=52 * 1024 * 1024),
            name='finish',
        )(hidden, w_out, o, ml)
        return h_out, k_upd.reshape(k_cache.shape), v_upd.reshape(v_cache.shape)

    return jax.shard_map(
        local_step,
        mesh=mesh,
        in_specs=(P('dp', None), P(None), P(None, 'tp'), P('tp', None), cache_spec, cache_spec, P('dp')),
        out_specs=(P('dp', None), cache_spec, cache_spec),
        check_vma=False,
    )
```

```python
import math

import jax
import jax.numpy as jnp
from jax import lax
from jax.experimental import pallas as pl
from jax.experimental.pallas import tpu as pltpu
from jax.sharding import PartitionSpec as P

MESH = pl.DeviceIdType.MESH
NEG = -1e30
PV_LAG = 4
W_HEADS = 6
PART = 8
OUT_CHUNKS = 8
LN_EPS = 1e-5


def quarters(n_seq):
    sp = lax.axis_index('sp')
    x, c = sp // 2, sp % 2
    q = n_seq // 4

    def start(xx, cc):
        return pl.multiple_of((xx * 2 + cc) * q, q)
    return [start(1 - x, c), start(1 - x, 1 - c), start(x, 1 - c), start(x, c)]


def insert_row(k_ref, v_ref, at_b, p, kn, vn):
    rows, head = k_ref.shape[1:]
    kv_local = rows // 128
    per = 16 // kv_local
    tile = jnp.clip(p // per, 0, rows // 16 - 1)
    at = pl.ds(pl.multiple_of(tile * 16, 16), 16)
    hit = lax.broadcasted_iota(jnp.int32, (16, head), 0) // kv_local == p - tile * per
    k_ref[at_b, at, :] = jnp.where(hit, kn, k_ref[at_b, at, :].astype(jnp.float32)).astype(jnp.bfloat16)
    v_ref[at_b, at, :] = jnp.where(hit, vn, v_ref[at_b, at, :].astype(jnp.float32)).astype(jnp.bfloat16)


def row_index(n_q, rows):
    kv_local = n_q // 4
    col = lax.broadcasted_iota(jnp.int32, (n_q, rows), 1)
    qg = lax.broadcasted_iota(jnp.int32, (n_q, rows), 0) // 4
    return jnp.where(col % kv_local == qg, col // kv_local, 1 << 20)


def attend_parts(parts, arrive, q_at, p_at, k_ref, v_ref, idx_ref, s_ref, out_at):
    scale = k_ref.shape[2] ** -0.5

    def scores(b, slot, k):
        s_ref[slot, k] = lax.dot_general(
            q_at(b).astype(jnp.bfloat16), k_ref[b], (((1,), (1,)), ((), ())),
            preferred_element_type=jnp.float32)

    arrive(0)
    for k, b in enumerate(parts[0]):
        scores(b, 0, k)
    for i, part in enumerate(parts):
        more = i + 1 < len(parts)
        if more:
            arrive(i + 1)
        held = [None] * len(part)
        for k in range(len(part) + PV_LAG):
            if k < len(part):
                if more:
                    scores(parts[i + 1][k], (i + 1) % 2, k)
                s = jnp.where(idx_ref[...] <= p_at(part[k]), s_ref[i % 2, k] * scale, NEG)
                m = jnp.max(s, axis=1, keepdims=True)
                e = jnp.exp(s - m)
                held[k] = (e.astype(jnp.bfloat16), m, jnp.sum(e, axis=1, keepdims=True))
            if k >= PV_LAG:
                b = part[k - PV_LAG]
                e, m, l = held[k - PV_LAG]
                out_at(b, jnp.dot(e, v_ref[b], preferred_element_type=jnp.float32), m, l)


def put_stats(tile, lane_id, k, m, l):
    return jnp.where(lane_id == k, m, jnp.where(lane_id == 64 + k, l, tile))


def first_kernel(pos_hbm, h_hbm, scale_hbm, w_ref, kc_ref, vc_ref,
                 k_ref, v_ref, pay0, pay1, pay2, q_own, kn_own, vn_own,
                 pos_ref, h_ref, scale_ref, w_buf, u_ref, q_ref, kn_ref, vn_ref,
                 ang_ref, idx_ref, s_ref,
                 in_sem, w_sem, k_sem, v_sem):
    n_seq, d_model = h_ref.shape
    rows = k_ref.shape[1]
    head = k_ref.shape[2]
    kv_local = w_ref.shape[1] // (6 * head)
    n_q = 4 * kv_local
    base = lax.axis_index('sp') * (rows // kv_local)
    starts = quarters(n_seq)
    q4 = n_seq // 4
    per_slot = q4 // PART

    w_chunks, _, w_cols = w_buf.shape

    small = [pltpu.make_async_copy(h_hbm, h_ref, in_sem.at[0]),
             pltpu.make_async_copy(scale_hbm, scale_ref, in_sem.at[1]),
             pltpu.make_async_copy(pos_hbm, pos_ref, in_sem.at[2])]
    for cp in small:
        cp.start()

    def w_copy(t):
        return pltpu.make_async_copy(w_ref.at[:, pl.ds(t * w_cols, w_cols)], w_buf.at[t], w_sem.at[t])

    def c_copies(i):
        src = pl.ds(starts[i // per_slot] + (i % per_slot) * PART, PART)
        dst = pl.ds(i * PART, PART)
        return (pltpu.make_async_copy(kc_ref.at[src], k_ref.at[dst], k_sem.at[i]),
                pltpu.make_async_copy(vc_ref.at[src], v_ref.at[dst], v_sem.at[i]))

    for t in range(w_chunks):
        w_copy(t).start()
    for i in range(3 * per_slot):
        for c in c_copies(i):
            c.start(priority=1)

    idx_ref[...] = row_index(n_q, rows)

    lane = lax.broadcasted_iota(jnp.int32, (1, head), 1)
    half = head // 2
    inv_freq = jnp.exp((lane % half).astype(jnp.float32) * (-2.0 * math.log(500000.0) / head))
    small[2].wait()

    def fill(b, _):
        ang_ref[pl.ds(b, 1), :] = jnp.full((1, head), pos_ref[b].astype(jnp.float32)) * inv_freq
        return 0
    lax.fori_loop(0, n_seq, fill, 0)
    cos = jnp.cos(ang_ref[...])
    sin = jnp.sin(ang_ref[...]) * jnp.where(lane < half, -1.0, 1.0)

    def rope(x):
        return (x * cos + pltpu.roll(x, half, 1) * sin).astype(jnp.bfloat16).astype(jnp.float32)

    small[0].wait()
    small[1].wait()
    blocks = d_model // 128
    total = jnp.zeros((n_seq, 128), jnp.float32)
    for i in range(blocks):
        total += h_ref[:, i * 128:(i + 1) * 128].astype(jnp.float32)
    mean = jnp.sum(total, axis=1, keepdims=True) * (1.0 / d_model)
    total = jnp.zeros((n_seq, 128), jnp.float32)
    for i in range(blocks):
        cen = h_ref[:, i * 128:(i + 1) * 128].astype(jnp.float32) - mean
        total += cen * cen
    var = jnp.sum(total, axis=1, keepdims=True) * (1.0 / d_model)
    rstd = lax.rsqrt(var + LN_EPS)
    for i in range(blocks):
        cen = h_ref[:, i * 128:(i + 1) * 128].astype(jnp.float32) - mean
        u_ref[:, i * 128:(i + 1) * 128] = (
            cen * rstd * scale_ref[i:i + 1, :].astype(jnp.float32)).astype(jnp.bfloat16)

    for t in range(w_chunks):
        w_copy(t).wait()
        acc = jnp.dot(u_ref[...], w_buf[t], preferred_element_type=jnp.float32)
        qkv = jnp.clip(acc.astype(jnp.bfloat16).astype(jnp.float32), -8.0, 8.0)
        for j in range(W_HEADS):
            g, kind = divmod(t * W_HEADS + j, 6)
            val = qkv[:, j * head:(j + 1) * head]
            if kind < 4:
                q_ref[:, g * 4 + kind, :] = rope(val)
                continue
            new_ref, new = (kn_ref, rope(val)) if kind == 4 else (vn_ref, val)
            for r in range(16 // kv_local):
                new_ref[:, r * kv_local + g, :] = new

    pays = [pay0, pay1, pay2]
    lane_id = lax.broadcasted_iota(jnp.int32, (n_q, 128), 1)
    stats = [jnp.zeros((n_q, 128), jnp.float32) for _ in pays]

    def seq(b):
        return starts[b // q4] + b % q4

    def arrive(i):
        for c in c_copies(i):
            c.wait()
        for k in range(PART):
            b = i * PART + k
            insert_row(k_ref, v_ref, b, pos_ref[seq(b)] - base, kn_ref[seq(b)], vn_ref[seq(b)])

    def out_at(b, o, m, l):
        pays[b // q4][b % q4] = o
        stats[b // q4] = put_stats(stats[b // q4], lane_id, b % q4, m, l)

    parts = [list(range(i * PART, (i + 1) * PART)) for i in range(3 * per_slot)]
    attend_parts(parts, arrive, lambda b: q_ref[seq(b)], lambda b: pos_ref[seq(b)] - base,
                 k_ref, v_ref, idx_ref, s_ref, out_at)
    for pay, tile in zip(pays, stats):
        pay[q4] = tile
    own = pl.ds(starts[3], q4)
    q_own[...] = q_ref[own]
    kn_own[...] = kn_ref[own]
    vn_own[...] = vn_ref[own]


def second_kernel(pos_hbm, q_ref, kn_ref, vn_ref, k3_ref, v3_ref, kc_ref, vc_ref,
                  ko_ref, vo_ref, pay_ref,
                  pos_ref, k_ref, v_ref, idx_ref, s_ref,
                  in_sem, k_sem, v_sem, o_sem, o3_sem):
    n_seq = ko_ref.shape[0]
    rows = k_ref.shape[1]
    n_q = q_ref.shape[1]
    base = lax.axis_index('sp') * (rows // (n_q // 4))
    starts = quarters(n_seq)
    q4 = n_seq // 4
    per_slot = q4 // PART

    pos_copy = pltpu.make_async_copy(pos_hbm, pos_ref, in_sem.at[0])
    pos_copy.start()

    def c_copies(i):
        src = pl.ds(starts[3] + i * PART, PART)
        dst = pl.ds(i * PART, PART)
        return (pltpu.make_async_copy(kc_ref.at[src], k_ref.at[dst], k_sem.at[i]),
                pltpu.make_async_copy(vc_ref.at[src], v_ref.at[dst], v_sem.at[i]))

    def o_copies(i):
        dst = pl.ds(starts[3] + i * PART, PART)
        src = pl.ds(i * PART, PART)
        return (pltpu.make_async_copy(k_ref.at[src], ko_ref.at[dst], o_sem.at[0, i]),
                pltpu.make_async_copy(v_ref.at[src], vo_ref.at[dst], o_sem.at[1, i]))

    def o3_copies(i):
        dst = pl.ds(starts[i], q4)
        src = pl.ds(i * q4, q4)
        return (pltpu.make_async_copy(k3_ref.at[src], ko_ref.at[dst], o3_sem.at[0, i]),
                pltpu.make_async_copy(v3_ref.at[src], vo_ref.at[dst], o3_sem.at[1, i]))

    for i in range(per_slot):
        for c in c_copies(i):
            c.start()
    for i in range(3):
        for c in o3_copies(i):
            c.start(priority=1)
    idx_ref[...] = row_index(n_q, rows)
    pos_copy.wait()

    lane_id = lax.broadcasted_iota(jnp.int32, (n_q, 128), 1)
    stats = [jnp.zeros((n_q, 128), jnp.float32)]

    def arrive(i):
        for c in c_copies(i):
            c.wait()
        for k in range(PART):
            b = i * PART + k
            insert_row(k_ref, v_ref, b, pos_ref[starts[3] + b] - base, kn_ref[b], vn_ref[b])
        for c in o_copies(i):
            c.start(priority=1)

    def out_at(b, o, m, l):
        pay_ref[b] = o
        stats[0] = put_stats(stats[0], lane_id, b, m, l)

    parts = [list(range(i * PART, (i + 1) * PART)) for i in range(per_slot)]
    attend_parts(parts, arrive, lambda b: q_ref[b], lambda b: pos_ref[starts[3] + b] - base,
                 k_ref, v_ref, idx_ref, s_ref, out_at)
    pay_ref[q4] = stats[0]
    for i in range(3):
        for c in o3_copies(i):
            c.wait()
    for i in range(per_slot):
        for c in o_copies(i):
            c.wait()


def finish_kernel(h_ref, w_ref, p0_ref, p1_ref, p2_ref, p3_ref, out_ref,
                  w_buf, att, att_send, lhs, part, y_in, fin, x_in, d_in, d_in2,
                  w_sem, a_sem, ys_sem, yr_sem, xs_sem, xr_sem, ds_sem, dr_sem, es_sem, er_sem):
    n_q = p0_ref.shape[1]
    sp = lax.axis_index('sp')
    tp = lax.axis_index('tp')
    x, c = sp // 2, sp % 2
    sib = {'sp': x * 2 + (1 - c)}
    xn = {'sp': (1 - x) * 2 + c}
    yn = {'tp': 1 - tp}

    half_cols = w_buf.shape[1]
    cc = half_cols // OUT_CHUNKS
    q4 = att_send.shape[0]
    own_col = c * half_cols
    oth_col = (1 - c) * half_cols

    def w_copy(j):
        return pltpu.make_async_copy(
            w_ref.at[:, pl.ds(pl.multiple_of(own_col + j * cc, 128), cc)],
            w_buf.at[:, pl.ds(j * cc, cc)], w_sem.at[j])

    for j in range(OUT_CHUNKS):
        w_copy(j).start()

    barrier = pltpu.get_barrier_semaphore()
    for dev in (sib, xn, yn):
        pl.semaphore_signal(barrier, inc=1, device_id=dev, device_id_type=MESH)

    def remote(src, dst, ssem, rsem, dev):
        return pltpu.make_async_remote_copy(src_ref=src, dst_ref=dst, send_sem=ssem, recv_sem=rsem,
                                            device_id=dev, device_id_type=MESH)

    pays = [p0_ref, p1_ref, p2_ref, p3_ref]
    maxes = [p[q4] for p in pays]
    sums = [pltpu.roll(m, 64, 1) for m in maxes]
    top = jnp.maximum(jnp.maximum(maxes[0], maxes[1]), jnp.maximum(maxes[2], maxes[3]))
    factors = [jnp.exp(m - top) for m in maxes]
    inv = 1.0 / sum(l * f for l, f in zip(sums, factors))
    factors = [f * inv for f in factors]
    for i in range(q4):
        att_send[i] = sum(p[i] * jnp.broadcast_to(f[:, i:i + 1], (n_q, 128)) for p, f in zip(pays, factors))

    pl.semaphore_wait(barrier, 3)
    c_att = remote(att_send, att, a_sem.at[0], a_sem.at[1], sib)
    c_att.start()
    for n in range(n_q):
        lhs[pl.ds(c * q4, q4), n * 128:(n + 1) * 128] = att_send[:, n, :].astype(jnp.bfloat16)
    c_att.wait_recv()
    for n in range(n_q):
        lhs[pl.ds((1 - c) * q4, q4), n * 128:(n + 1) * 128] = att[:, n, :].astype(jnp.bfloat16)

    y_copy, x_copy, d_copy, e_copy = [], [], [], []
    for j in range(OUT_CHUNKS):
        w_copy(j).wait()
        part[j] = jnp.dot(lhs[...], w_buf[:, j * cc:(j + 1) * cc], preferred_element_type=jnp.float32)
        y_copy.append(remote(part.at[j], y_in.at[j], ys_sem.at[j], yr_sem.at[j], yn))
        y_copy[j].start()

    my_rows = pl.ds(pl.multiple_of(x * (2 * q4), 2 * q4), 2 * q4)
    xn_rows = pl.ds(pl.multiple_of((1 - x) * (2 * q4), 2 * q4), 2 * q4)

    def cols(start, j):
        return pl.ds(pl.multiple_of(start + j * cc, 128), cc)

    for j in range(OUT_CHUNKS):
        y_copy[j].wait_recv()
        fin[j] = h_ref[my_rows, cols(own_col, j)].astype(jnp.float32) + (part[j] + y_in[j])
        x_copy.append(remote(fin.at[j], x_in.at[j], xs_sem.at[j], xr_sem.at[j], xn))
        x_copy[j].start()
        d_copy.append(remote(fin.at[j], d_in.at[j], ds_sem.at[j], dr_sem.at[j], sib))
        d_copy[j].start()
        out_ref[my_rows, cols(own_col, j)] = fin[j].astype(jnp.bfloat16)
    for j in range(OUT_CHUNKS):
        x_copy[j].wait_recv()
        e_copy.append(remote(x_in.at[j], d_in2.at[j], es_sem.at[j], er_sem.at[j], sib))
        e_copy[j].start()
        out_ref[xn_rows, cols(own_col, j)] = x_in[j].astype(jnp.bfloat16)
        d_copy[j].wait_recv()
        out_ref[my_rows, cols(oth_col, j)] = d_in[j].astype(jnp.bfloat16)
    for j in range(OUT_CHUNKS):
        e_copy[j].wait_recv()
        out_ref[xn_rows, cols(oth_col, j)] = d_in2[j].astype(jnp.bfloat16)

    for cp in [c_att] + y_copy + x_copy + d_copy + e_copy:
        cp.wait_send()


def solution(mesh):
    cache_spec = P('dp', 'sp', 'tp', None)

    def local_step(hidden, norm_scale, w_qkv, w_out, k_cache, v_cache, positions):
        n_seq, seq_local, kv_local, head = k_cache.shape
        d_model = hidden.shape[1]
        rows = seq_local * kv_local
        n_q = 4 * kv_local
        q4 = n_seq // 4
        vm = pl.BlockSpec(memory_space=pltpu.VMEM)
        hbm = pl.BlockSpec(memory_space=pltpu.HBM)
        dma = pltpu.SemaphoreType.DMA
        f32, bf16 = jnp.float32, jnp.bfloat16
        payload = pltpu.VMEM((q4 + 1, n_q, head), f32)
        k_rows = k_cache.reshape(n_seq, rows, head)
        v_rows = v_cache.reshape(n_seq, rows, head)
        slots = 3 * q4 // PART

        def pin(a):
            return pltpu.with_memory_space_constraint(a, pltpu.HBM)

        k3, v3, pay0, pay1, pay2, q_own, kn_own, vn_own = pl.pallas_call(
            first_kernel,
            out_shape=(pltpu.VMEM((3 * q4, rows, head), bf16), pltpu.VMEM((3 * q4, rows, head), bf16),
                       payload, payload, payload,
                       pltpu.VMEM((q4, n_q, head), f32), pltpu.VMEM((q4, 16, head), f32),
                       pltpu.VMEM((q4, 16, head), f32)),
            in_specs=[hbm] * 6,
            out_specs=(vm,) * 8,
            scratch_shapes=[
                pltpu.SMEM((n_seq,), jnp.int32),
                pltpu.VMEM((n_seq, d_model), bf16),
                pltpu.VMEM((d_model // 128, 128), bf16),
                pltpu.VMEM((6 * kv_local // W_HEADS, d_model, W_HEADS * head), bf16),
                pltpu.VMEM((n_seq, d_model), bf16),
                pltpu.VMEM((n_seq, n_q, head), f32),
                pltpu.VMEM((n_seq, 16, head), f32),
                pltpu.VMEM((n_seq, 16, head), f32),
                pltpu.VMEM((n_seq, head), f32),
                pltpu.VMEM((n_q, rows), jnp.int32),
                pltpu.VMEM((2, PART, n_q, rows), f32),
                dma((3,)), dma((6 * kv_local // W_HEADS,)), dma((slots,)), dma((slots,)),
            ],
            compiler_params=pltpu.CompilerParams(vmem_limit_bytes=40 * 1024 * 1024),
            cost_estimate=pl.CostEstimate(flops=2 * 10**10, bytes_accessed=4 * 10**7, transcendentals=0),
            name='first',
        )(*map(pin, (positions, hidden, norm_scale.reshape(d_model // 128, 128), w_qkv, k_rows, v_rows)))

        got0 = lax.ppermute(pay0, 'sp', [(i, i ^ 2) for i in range(4)])
        got1 = lax.ppermute(pay1, 'sp', [(i, 3 - i) for i in range(4)])
        got2 = lax.ppermute(pay2, 'sp', [(i, i ^ 1) for i in range(4)])

        k_upd, v_upd, mine = pl.pallas_call(
            second_kernel,
            out_shape=(jax.ShapeDtypeStruct((n_seq, rows, head), bf16),
                       jax.ShapeDtypeStruct((n_seq, rows, head), bf16), payload),
            in_specs=[hbm, vm, vm, vm, vm, vm, hbm, hbm],
            out_specs=(hbm, hbm, vm),
            scratch_shapes=[
                pltpu.SMEM((n_seq,), jnp.int32),
                pltpu.VMEM((q4, rows, head), bf16),
                pltpu.VMEM((q4, rows, head), bf16),
                pltpu.VMEM((n_q, rows), jnp.int32),
                pltpu.VMEM((2, PART, n_q, rows), f32),
                dma((1,)), dma((q4 // PART,)), dma((q4 // PART,)), dma((2, q4 // PART)), dma((2, 3)),
            ],
            compiler_params=pltpu.CompilerParams(vmem_limit_bytes=40 * 1024 * 1024),
            cost_estimate=pl.CostEstimate(flops=2 * 10**10, bytes_accessed=4 * 10**7, transcendentals=0),
            name='second',
        )(pin(positions), q_own, kn_own, vn_own, k3, v3, pin(k_rows), pin(v_rows))

        half_cols = d_model // 2
        cc = half_cols // OUT_CHUNKS
        chunk = pltpu.VMEM((OUT_CHUNKS, 2 * q4, cc), f32)
        h_out = pl.pallas_call(
            finish_kernel,
            out_shape=jax.ShapeDtypeStruct((n_seq, d_model), bf16),
            in_specs=[vm, hbm, vm, vm, vm, vm],
            out_specs=vm,
            scratch_shapes=[
                pltpu.VMEM((w_out.shape[0], half_cols), bf16),
                pltpu.VMEM((q4, n_q, head), f32),
                pltpu.VMEM((q4, n_q, head), f32),
                pltpu.VMEM((2 * q4, n_q * head), bf16),
                chunk, chunk, chunk, chunk, chunk, chunk,
                dma((OUT_CHUNKS,)), dma((2,)),
                dma((OUT_CHUNKS,)), dma((OUT_CHUNKS,)),
                dma((OUT_CHUNKS,)), dma((OUT_CHUNKS,)),
                dma((OUT_CHUNKS,)), dma((OUT_CHUNKS,)),
                dma((OUT_CHUNKS,)), dma((OUT_CHUNKS,)),
            ],
            compiler_params=pltpu.CompilerParams(
                collective_id=0, has_side_effects=True, vmem_limit_bytes=50 * 1024 * 1024),
            name='finish',
        )(hidden, pin(w_out), mine, got0, got1, got2)
        return h_out, k_upd.reshape(k_cache.shape), v_upd.reshape(v_cache.shape)

    return jax.shard_map(
        local_step,
        mesh=mesh,
        in_specs=(P('dp', None), P(None), P(None, 'tp'), P('tp', None), cache_spec, cache_spec, P('dp')),
        out_specs=(P('dp', None), cache_spec, cache_spec),
        check_vma=False,
    )
```

```python
import math

import jax
import jax.numpy as jnp
from jax import lax
from jax.experimental import pallas as pl
from jax.experimental.pallas import tpu as pltpu
from jax.sharding import PartitionSpec as P

MESH = pl.DeviceIdType.MESH
NEG = -1e30
PV_LAG = 4
W_HEADS = 6
PART = 8
OUT_CHUNKS = 8
LN_EPS = 1e-5
FIRST_VMEM = 36


def quarters(n_seq):
    sp = lax.axis_index('sp')
    x, c = sp // 2, sp % 2
    q = n_seq // 4

    def start(xx, cc):
        return pl.multiple_of((xx * 2 + cc) * q, q)
    return [start(1 - x, c), start(1 - x, 1 - c), start(x, 1 - c), start(x, c)]


def insert_row(k_ref, v_ref, at_b, p, kn, vn):
    rows, head = k_ref.shape[1:]
    kv_local = rows // 128
    per = 16 // kv_local
    tile = jnp.clip(p // per, 0, rows // 16 - 1)
    at = pl.ds(pl.multiple_of(tile * 16, 16), 16)
    hit = lax.broadcasted_iota(jnp.int32, (16, head), 0) // kv_local == p - tile * per
    k_ref[at_b, at, :] = jnp.where(hit, kn, k_ref[at_b, at, :].astype(jnp.float32)).astype(jnp.bfloat16)
    v_ref[at_b, at, :] = jnp.where(hit, vn, v_ref[at_b, at, :].astype(jnp.float32)).astype(jnp.bfloat16)


def row_index(n_q, rows):
    kv_local = n_q // 4
    col = lax.broadcasted_iota(jnp.int32, (n_q, rows), 1)
    qg = lax.broadcasted_iota(jnp.int32, (n_q, rows), 0) // 4
    return jnp.where(col % kv_local == qg, col // kv_local, 1 << 20)


def attend_parts(parts, arrive, q_at, p_at, k_ref, v_ref, idx_ref, s_ref, out_at):
    scale = k_ref.shape[2] ** -0.5

    def scores(b, slot, k):
        s_ref[slot, k] = lax.dot_general(
            q_at(b).astype(jnp.bfloat16), k_ref[b], (((1,), (1,)), ((), ())),
            preferred_element_type=jnp.float32)

    arrive(0)
    for k, b in enumerate(parts[0]):
        scores(b, 0, k)
    for i, part in enumerate(parts):
        more = i + 1 < len(parts)
        if more:
            arrive(i + 1)
        held = [None] * len(part)
        for k in range(len(part) + PV_LAG):
            if k < len(part):
                if more:
                    scores(parts[i + 1][k], (i + 1) % 2, k)
                s = jnp.where(idx_ref[...] <= p_at(part[k]), s_ref[i % 2, k] * scale, NEG)
                m = jnp.max(s, axis=1, keepdims=True)
                e = jnp.exp(s - m)
                held[k] = (e.astype(jnp.bfloat16), m, jnp.sum(e, axis=1, keepdims=True))
            if k >= PV_LAG:
                b = part[k - PV_LAG]
                e, m, l = held[k - PV_LAG]
                out_at(b, jnp.dot(e, v_ref[b], preferred_element_type=jnp.float32), m, l)


def put_stats(tile, lane_id, k, m, l):
    return jnp.where(lane_id == k, m, jnp.where(lane_id == 64 + k, l, tile))


def first_kernel(pos_hbm, h_hbm, scale_hbm, w_ref, kc_ref, vc_ref,
                 k_ref, v_ref, pay0, pay1, pay2, q_own, kn_ref, vn_ref,
                 pos_ref, h_ref, scale_ref, w_buf, u_ref, qkv_ref, q_ref,
                 ang_ref, idx_ref, s_ref,
                 in_sem, w_sem, k_sem, v_sem, send_sem, recv_sem):
    n_seq, d_model = h_ref.shape
    rows = k_ref.shape[1]
    head = k_ref.shape[2]
    w_chunks, _, w_cols = w_buf.shape
    n_q = q_ref.shape[1]
    kv_local = n_q // 4
    sp = lax.axis_index('sp')
    core = sp % 2
    sib = {'sp': sp + 1 - 2 * core}
    base = sp * (rows // kv_local)
    starts = quarters(n_seq)
    q4 = n_seq // 4
    per_slot = q4 // PART

    small = [pltpu.make_async_copy(h_hbm, h_ref, in_sem.at[0]),
             pltpu.make_async_copy(scale_hbm, scale_ref, in_sem.at[1]),
             pltpu.make_async_copy(pos_hbm, pos_ref, in_sem.at[2])]
    for cp in small:
        cp.start()

    def w_copy(t):
        at = pl.multiple_of((core * w_chunks + t) * w_cols, 128)
        return pltpu.make_async_copy(w_ref.at[:, pl.ds(at, w_cols)], w_buf.at[t], w_sem.at[t])

    def c_copies(i):
        src = pl.ds(starts[i // per_slot] + (i % per_slot) * PART, PART)
        dst = pl.ds(i * PART, PART)
        return (pltpu.make_async_copy(kc_ref.at[src], k_ref.at[dst], k_sem.at[i]),
                pltpu.make_async_copy(vc_ref.at[src], v_ref.at[dst], v_sem.at[i]))

    for t in range(w_chunks):
        w_copy(t).start()
    for i in range(4 * per_slot):
        for c in c_copies(i):
            c.start(priority=1)

    barrier = pltpu.get_barrier_semaphore()
    pl.semaphore_signal(barrier, inc=1, device_id=sib, device_id_type=MESH)

    idx_ref[...] = row_index(n_q, rows)

    lane = lax.broadcasted_iota(jnp.int32, (1, head), 1)
    half = head // 2
    inv_freq = jnp.exp((lane % half).astype(jnp.float32) * (-2.0 * math.log(500000.0) / head))
    small[2].wait()

    def fill(b, _):
        ang_ref[pl.ds(b, 1), :] = jnp.full((1, head), pos_ref[b].astype(jnp.float32)) * inv_freq
        return 0
    lax.fori_loop(0, n_seq, fill, 0)
    cos = jnp.cos(ang_ref[...])
    sin = jnp.sin(ang_ref[...]) * jnp.where(lane < half, -1.0, 1.0)

    def rope(x):
        return (x * cos + pltpu.roll(x, half, 1) * sin).astype(jnp.bfloat16).astype(jnp.float32)

    small[0].wait()
    small[1].wait()
    blocks = d_model // 128
    total = jnp.zeros((n_seq, 128), jnp.float32)
    for i in range(blocks):
        total += h_ref[:, i * 128:(i + 1) * 128].astype(jnp.float32)
    mean = jnp.sum(total, axis=1, keepdims=True) * (1.0 / d_model)
    total = jnp.zeros((n_seq, 128), jnp.float32)
    for i in range(blocks):
        cen = h_ref[:, i * 128:(i + 1) * 128].astype(jnp.float32) - mean
        total += cen * cen
    var = jnp.sum(total, axis=1, keepdims=True) * (1.0 / d_model)
    rstd = lax.rsqrt(var + LN_EPS)
    for i in range(blocks):
        cen = h_ref[:, i * 128:(i + 1) * 128].astype(jnp.float32) - mean
        u_ref[:, i * 128:(i + 1) * 128] = (
            cen * rstd * scale_ref[i:i + 1, :].astype(jnp.float32)).astype(jnp.bfloat16)
    pl.semaphore_wait(barrier, 1)

    heads = w_cols // head
    sends = []
    for t in range(w_chunks):
        w_copy(t).wait()
        acc = jnp.dot(u_ref[...], w_buf[t], preferred_element_type=jnp.float32)
        qkv = jnp.clip(acc.astype(jnp.bfloat16).astype(jnp.float32), -8.0, 8.0)
        at = (core * w_chunks + t) * heads
        for j in range(heads):
            val = qkv[:, j * head:(j + 1) * head]
            qkv_ref[at + j] = rope(val) if j % 6 < 5 else val
        block = qkv_ref.at[pl.ds(at, heads)]
        sends.append(pltpu.make_async_remote_copy(
            src_ref=block, dst_ref=block, send_sem=send_sem.at[t], recv_sem=recv_sem.at[t],
            device_id=sib, device_id_type=MESH))
        sends[t].start()
    for cp in sends:
        cp.wait_recv()
    for g in range(kv_local):
        for j in range(4):
            q_ref[:, g * 4 + j, :] = qkv_ref[g * 6 + j]
        for r in range(16 // kv_local):
            kn_ref[:, r * kv_local + g, :] = qkv_ref[g * 6 + 4]
            vn_ref[:, r * kv_local + g, :] = qkv_ref[g * 6 + 5]

    pays = [pay0, pay1, pay2]
    lane_id = lax.broadcasted_iota(jnp.int32, (n_q, 128), 1)
    stats = [jnp.zeros((n_q, 128), jnp.float32) for _ in pays]

    def seq(b):
        return starts[b // q4] + b % q4

    def arrive(i):
        for c in c_copies(i):
            c.wait()

    def out_at(b, o, m, l):
        pays[b // q4][b % q4] = o
        stats[b // q4] = put_stats(stats[b // q4], lane_id, b % q4, m, l)

    parts = [list(range(i * PART, (i + 1) * PART)) for i in range(3 * per_slot)]
    attend_parts(parts, arrive, lambda b: q_ref[seq(b)], lambda b: pos_ref[seq(b)] - base - 1,
                 k_ref, v_ref, idx_ref, s_ref, out_at)
    for pay, tile in zip(pays, stats):
        pay[q4] = tile
    q_own[...] = q_ref[pl.ds(starts[3], q4)]
    for i in range(3 * per_slot, 4 * per_slot):
        arrive(i)
    for cp in sends:
        cp.wait_send()


def second_kernel(pos_hbm, q_ref, kn_ref, vn_ref, k_in, v_in,
                  ko_ref, vo_ref, pay_ref, k_ref, v_ref,
                  pos_ref, idx_ref, s_ref,
                  in_sem, o_sem):
    n_seq, rows, head = k_ref.shape
    n_q = q_ref.shape[1]
    kv_local = n_q // 4
    base = lax.axis_index('sp') * (rows // kv_local)
    starts = quarters(n_seq)
    q4 = n_seq // 4

    pos_copy = pltpu.make_async_copy(pos_hbm, pos_ref, in_sem.at[0])
    pos_copy.start()
    idx_ref[...] = row_index(n_q, rows)
    pos_copy.wait()

    def o_copies(i):
        dst = pl.ds(starts[i], q4)
        src = pl.ds(i * q4, q4)
        return (pltpu.make_async_copy(k_ref.at[src], ko_ref.at[dst], o_sem.at[0, i]),
                pltpu.make_async_copy(v_ref.at[src], vo_ref.at[dst], o_sem.at[1, i]))

    for i in range(4):
        for k in range(q4):
            b = starts[i] + k
            insert_row(k_ref, v_ref, i * q4 + k, pos_ref[b] - base, kn_ref[b], vn_ref[b])
        for c in o_copies(i):
            c.start()

    lane_id = lax.broadcasted_iota(jnp.int32, (n_q, 128), 1)
    stats = [jnp.zeros((n_q, 128), jnp.float32)]

    def per_head(tile):
        return jnp.concatenate([jnp.broadcast_to(tile[g:g + 1], (4, head)) for g in range(kv_local)], axis=0)

    def out_at(b, o, m, l):
        k = b - 3 * q4
        at = starts[3] + k
        s = jnp.sum(q_ref[k] * per_head(kn_ref[at]), axis=1, keepdims=True) * head ** -0.5
        top = jnp.maximum(m, s)
        old, new = jnp.exp(m - top), jnp.exp(s - top)
        pay_ref[k] = o * old + new.astype(jnp.bfloat16).astype(jnp.float32) * per_head(vn_ref[at])
        stats[0] = put_stats(stats[0], lane_id, k, top, l * old + new)

    parts = [list(range(3 * q4 + i, 3 * q4 + i + PART)) for i in range(0, q4, PART)]
    attend_parts(parts, lambda i: None, lambda b: q_ref[b - 3 * q4],
                 lambda b: pos_ref[starts[3] + b - 3 * q4] - base - 1,
                 k_ref, v_ref, idx_ref, s_ref, out_at)
    pay_ref[q4] = stats[0]
    for i in range(4):
        for c in o_copies(i):
            c.wait()


def finish_kernel(h_ref, w_ref, p0_ref, p1_ref, p2_ref, p3_ref, out_ref,
                  w_buf, att, att_send, lhs, part, y_in, fin, x_in, d_in, d_in2,
                  w_sem, a_sem, ys_sem, yr_sem, xs_sem, xr_sem, ds_sem, dr_sem, es_sem, er_sem):
    n_q = p0_ref.shape[1]
    sp = lax.axis_index('sp')
    tp = lax.axis_index('tp')
    x, c = sp // 2, sp % 2
    sib = {'sp': x * 2 + (1 - c)}
    xn = {'sp': (1 - x) * 2 + c}
    yn = {'tp': 1 - tp}

    half_cols = w_buf.shape[1]
    cc = half_cols // OUT_CHUNKS
    q4 = att_send.shape[0]
    own_col = c * half_cols
    oth_col = (1 - c) * half_cols

    def w_copy(j):
        return pltpu.make_async_copy(
            w_ref.at[:, pl.ds(pl.multiple_of(own_col + j * cc, 128), cc)],
            w_buf.at[:, pl.ds(j * cc, cc)], w_sem.at[j])

    for j in range(OUT_CHUNKS):
        w_copy(j).start()

    barrier = pltpu.get_barrier_semaphore()
    for dev in (sib, xn, yn):
        pl.semaphore_signal(barrier, inc=1, device_id=dev, device_id_type=MESH)

    def remote(src, dst, ssem, rsem, dev):
        return pltpu.make_async_remote_copy(src_ref=src, dst_ref=dst, send_sem=ssem, recv_sem=rsem,
                                            device_id=dev, device_id_type=MESH)

    pays = [p0_ref, p1_ref, p2_ref, p3_ref]
    maxes = [p[q4] for p in pays]
    sums = [pltpu.roll(m, 64, 1) for m in maxes]
    top = jnp.maximum(jnp.maximum(maxes[0], maxes[1]), jnp.maximum(maxes[2], maxes[3]))
    factors = [jnp.exp(m - top) for m in maxes]
    inv = 1.0 / sum(l * f for l, f in zip(sums, factors))
    factors = [f * inv for f in factors]
    for i in range(q4):
        att_send[i] = sum(p[i] * jnp.broadcast_to(f[:, i:i + 1], (n_q, 128)) for p, f in zip(pays, factors))

    pl.semaphore_wait(barrier, 3)
    c_att = remote(att_send, att, a_sem.at[0], a_sem.at[1], sib)
    c_att.start()
    for n in range(n_q):
        lhs[pl.ds(c * q4, q4), n * 128:(n + 1) * 128] = att_send[:, n, :].astype(jnp.bfloat16)
    c_att.wait_recv()
    for n in range(n_q):
        lhs[pl.ds((1 - c) * q4, q4), n * 128:(n + 1) * 128] = att[:, n, :].astype(jnp.bfloat16)

    y_copy, x_copy, d_copy, e_copy = [], [], [], []
    for j in range(OUT_CHUNKS):
        w_copy(j).wait()
        part[j] = jnp.dot(lhs[...], w_buf[:, j * cc:(j + 1) * cc], preferred_element_type=jnp.float32)
        y_copy.append(remote(part.at[j], y_in.at[j], ys_sem.at[j], yr_sem.at[j], yn))
        y_copy[j].start()

    my_rows = pl.ds(pl.multiple_of(x * (2 * q4), 2 * q4), 2 * q4)
    xn_rows = pl.ds(pl.multiple_of((1 - x) * (2 * q4), 2 * q4), 2 * q4)

    def cols(start, j):
        return pl.ds(pl.multiple_of(start + j * cc, 128), cc)

    for j in range(OUT_CHUNKS):
        y_copy[j].wait_recv()
        fin[j] = h_ref[my_rows, cols(own_col, j)].astype(jnp.float32) + (part[j] + y_in[j])
        x_copy.append(remote(fin.at[j], x_in.at[j], xs_sem.at[j], xr_sem.at[j], xn))
        x_copy[j].start()
        d_copy.append(remote(fin.at[j], d_in.at[j], ds_sem.at[j], dr_sem.at[j], sib))
        d_copy[j].start()
        out_ref[my_rows, cols(own_col, j)] = fin[j].astype(jnp.bfloat16)
    for j in range(OUT_CHUNKS):
        x_copy[j].wait_recv()
        e_copy.append(remote(x_in.at[j], d_in2.at[j], es_sem.at[j], er_sem.at[j], sib))
        e_copy[j].start()
        out_ref[xn_rows, cols(own_col, j)] = x_in[j].astype(jnp.bfloat16)
        d_copy[j].wait_recv()
        out_ref[my_rows, cols(oth_col, j)] = d_in[j].astype(jnp.bfloat16)
    for j in range(OUT_CHUNKS):
        e_copy[j].wait_recv()
        out_ref[xn_rows, cols(oth_col, j)] = d_in2[j].astype(jnp.bfloat16)

    for cp in [c_att] + y_copy + x_copy + d_copy + e_copy:
        cp.wait_send()


def solution(mesh):
    cache_spec = P('dp', 'sp', 'tp', None)

    def local_step(hidden, norm_scale, w_qkv, w_out, k_cache, v_cache, positions):
        n_seq, seq_local, kv_local, head = k_cache.shape
        d_model = hidden.shape[1]
        rows = seq_local * kv_local
        n_q = 4 * kv_local
        q4 = n_seq // 4
        vm = pl.BlockSpec(memory_space=pltpu.VMEM)
        hbm = pl.BlockSpec(memory_space=pltpu.HBM)
        dma = pltpu.SemaphoreType.DMA
        f32, bf16 = jnp.float32, jnp.bfloat16
        payload = pltpu.VMEM((q4 + 1, n_q, head), f32)
        k_rows = k_cache.reshape(n_seq, rows, head)
        v_rows = v_cache.reshape(n_seq, rows, head)
        slots = n_seq // PART

        def pin(a):
            return pltpu.with_memory_space_constraint(a, pltpu.HBM)

        k_all, v_all, pay0, pay1, pay2, q_own, kn, vn = pl.pallas_call(
            first_kernel,
            out_shape=(pltpu.VMEM((n_seq, rows, head), bf16), pltpu.VMEM((n_seq, rows, head), bf16),
                       payload, payload, payload,
                       pltpu.VMEM((q4, n_q, head), f32), pltpu.VMEM((n_seq, 16, head), f32),
                       pltpu.VMEM((n_seq, 16, head), f32)),
            in_specs=[hbm] * 6,
            out_specs=(vm,) * 8,
            scratch_shapes=[
                pltpu.SMEM((n_seq,), jnp.int32),
                pltpu.VMEM((n_seq, d_model), bf16),
                pltpu.VMEM((d_model // 128, 128), bf16),
                pltpu.VMEM((3 * kv_local // W_HEADS, d_model, W_HEADS * head), bf16),
                pltpu.VMEM((n_seq, d_model), bf16),
                pltpu.VMEM((6 * kv_local, n_seq, head), f32),
                pltpu.VMEM((n_seq, n_q, head), f32),
                pltpu.VMEM((n_seq, head), f32),
                pltpu.VMEM((n_q, rows), jnp.int32),
                pltpu.VMEM((2, PART, n_q, rows), f32),
                dma((3,)), dma((3 * kv_local // W_HEADS,)), dma((slots,)), dma((slots,)),
                dma((3 * kv_local // W_HEADS,)), dma((3 * kv_local // W_HEADS,)),
            ],
            compiler_params=pltpu.CompilerParams(
                collective_id=1, has_side_effects=True, vmem_limit_bytes=FIRST_VMEM * 1024 * 1024),
            cost_estimate=pl.CostEstimate(flops=2 * 10**10, bytes_accessed=4 * 10**7, transcendentals=0),
            name='first',
        )(*map(pin, (positions, hidden, norm_scale.reshape(d_model // 128, 128), w_qkv, k_rows, v_rows)))

        got0 = lax.ppermute(pay0, 'sp', [(i, i ^ 2) for i in range(4)])
        got1 = lax.ppermute(pay1, 'sp', [(i, 3 - i) for i in range(4)])
        got2 = lax.ppermute(pay2, 'sp', [(i, i ^ 1) for i in range(4)])

        k_upd, v_upd, mine, _, _ = pl.pallas_call(
            second_kernel,
            out_shape=(jax.ShapeDtypeStruct((n_seq, rows, head), bf16),
                       jax.ShapeDtypeStruct((n_seq, rows, head), bf16), payload,
                       pltpu.VMEM((n_seq, rows, head), bf16), pltpu.VMEM((n_seq, rows, head), bf16)),
            in_specs=[hbm, vm, vm, vm, vm, vm],
            out_specs=(hbm, hbm, vm, vm, vm),
            input_output_aliases={4: 3, 5: 4},
            scratch_shapes=[
                pltpu.SMEM((n_seq,), jnp.int32),
                pltpu.VMEM((n_q, rows), jnp.int32),
                pltpu.VMEM((2, PART, n_q, rows), f32),
                dma((1,)), dma((2, 4)),
            ],
            compiler_params=pltpu.CompilerParams(vmem_limit_bytes=FIRST_VMEM * 1024 * 1024),
            cost_estimate=pl.CostEstimate(flops=2 * 10**10, bytes_accessed=4 * 10**7, transcendentals=0),
            name='second',
        )(pin(positions), q_own, kn, vn, k_all, v_all)

        half_cols = d_model // 2
        cc = half_cols // OUT_CHUNKS
        chunk = pltpu.VMEM((OUT_CHUNKS, 2 * q4, cc), f32)
        h_out = pl.pallas_call(
            finish_kernel,
            out_shape=jax.ShapeDtypeStruct((n_seq, d_model), bf16),
            in_specs=[vm, hbm, vm, vm, vm, vm],
            out_specs=vm,
            scratch_shapes=[
                pltpu.VMEM((w_out.shape[0], half_cols), bf16),
                pltpu.VMEM((q4, n_q, head), f32),
                pltpu.VMEM((q4, n_q, head), f32),
                pltpu.VMEM((2 * q4, n_q * head), bf16),
                chunk, chunk, chunk, chunk, chunk, chunk,
                dma((OUT_CHUNKS,)), dma((2,)),
                dma((OUT_CHUNKS,)), dma((OUT_CHUNKS,)),
                dma((OUT_CHUNKS,)), dma((OUT_CHUNKS,)),
                dma((OUT_CHUNKS,)), dma((OUT_CHUNKS,)),
                dma((OUT_CHUNKS,)), dma((OUT_CHUNKS,)),
            ],
            compiler_params=pltpu.CompilerParams(
                collective_id=0, has_side_effects=True, vmem_limit_bytes=50 * 1024 * 1024),
            name='finish',
        )(hidden, pin(w_out), mine, got0, got1, got2)
        return h_out, k_upd.reshape(k_cache.shape), v_upd.reshape(v_cache.shape)

    return jax.shard_map(
        local_step,
        mesh=mesh,
        in_specs=(P('dp', None), P(None), P(None, 'tp'), P('tp', None), cache_spec, cache_spec, P('dp')),
        out_specs=(P('dp', None), cache_spec, cache_spec),
        check_vma=False,
    )
```

```python
import math

import jax
import jax.numpy as jnp
from jax import lax
from jax.experimental import pallas as pl
from jax.experimental.pallas import tpu as pltpu
from jax.sharding import PartitionSpec as P

MESH = pl.DeviceIdType.MESH
NEG = -1e30
PV_LAG = 4
W_HEADS = 4
PART = 8
EARLY_PARTS = 6
OUT_CHUNKS = 8
LN_EPS = 1e-5
FIRST_VMEM = 36


def quarters(n_seq):
    sp = lax.axis_index('sp')
    x, c = sp // 2, sp % 2
    q = n_seq // 4

    def start(xx, cc):
        return pl.multiple_of((xx * 2 + cc) * q, q)
    own = start(x, 0)
    return [start(1 - x, 1 - c), start(1 - x, c), own, pl.multiple_of(own + q, q)]


def insert_row(k_ref, v_ref, at_b, p, kn, vn):
    rows, head = k_ref.shape[1:]
    kv_local = rows // 128
    per = 16 // kv_local
    tile = jnp.clip(p // per, 0, rows // 16 - 1)
    at = pl.ds(pl.multiple_of(tile * 16, 16), 16)
    hit = lax.broadcasted_iota(jnp.int32, (16, head), 0) // kv_local == p - tile * per
    k_ref[at_b, at, :] = jnp.where(hit, kn, k_ref[at_b, at, :].astype(jnp.float32)).astype(jnp.bfloat16)
    v_ref[at_b, at, :] = jnp.where(hit, vn, v_ref[at_b, at, :].astype(jnp.float32)).astype(jnp.bfloat16)


def write_copies(i, starts, q4, k_ref, v_ref, ko_ref, vo_ref, sem, first=0):
    at = i * PART
    src = pl.ds(at - first * PART, PART)
    dst = pl.ds(starts[at // q4] + at % q4, PART)
    return (pltpu.make_async_copy(k_ref.at[src], ko_ref.at[dst], sem.at[0, i]),
            pltpu.make_async_copy(v_ref.at[src], vo_ref.at[dst], sem.at[1, i]))


def insert_part(i, starts, base, pos_ref, k_ref, v_ref, kn_ref, vn_ref):
    q4 = k_ref.shape[0] // 4
    for k in range(i * PART, (i + 1) * PART):
        b = starts[k // q4] + k % q4
        insert_row(k_ref, v_ref, k, pos_ref[b] - base, kn_ref[b], vn_ref[b])


def row_index(n_q, rows):
    kv_local = n_q // 4
    col = lax.broadcasted_iota(jnp.int32, (n_q, rows), 1)
    qg = lax.broadcasted_iota(jnp.int32, (n_q, rows), 0) // 4
    return jnp.where(col % kv_local == qg, col // kv_local, 1 << 20)


def attend_parts(parts, arrive, q_at, p_at, k_ref, v_ref, idx_ref, s_ref, out_at):
    scale = k_ref.shape[2] ** -0.5

    def scores(b, slot, k):
        s_ref[slot, k] = lax.dot_general(
            q_at(b).astype(jnp.bfloat16), k_ref[b], (((1,), (1,)), ((), ())),
            preferred_element_type=jnp.float32)

    arrive(0)
    for k, b in enumerate(parts[0]):
        scores(b, 0, k)
    for i, part in enumerate(parts):
        more = i + 1 < len(parts)
        if more:
            arrive(i + 1)
        held = [None] * len(part)
        for k in range(len(part) + PV_LAG):
            if k < len(part):
                if more:
                    scores(parts[i + 1][k], (i + 1) % 2, k)
                s = jnp.where(idx_ref[...] <= p_at(part[k]), s_ref[i % 2, k] * scale, NEG)
                m = jnp.max(s, axis=1, keepdims=True)
                e = jnp.exp(s - m)
                held[k] = (e.astype(jnp.bfloat16), m, jnp.sum(e, axis=1, keepdims=True))
            if k >= PV_LAG:
                b = part[k - PV_LAG]
                e, m, l = held[k - PV_LAG]
                out_at(b, jnp.dot(e, v_ref[b], preferred_element_type=jnp.float32), m, l)


def put_stats(tile, lane_id, k, m, l):
    return jnp.where(lane_id == k, m, jnp.where(lane_id == 64 + k, l, tile))


def first_kernel(pos_hbm, h_hbm, scale_hbm, w_ref, kc_ref, vc_ref,
                 k_ref, v_ref, pay_ref, q_own, kn_ref, vn_ref,
                 pos_ref, h_ref, scale_ref, w_buf, u_ref, qkv_ref, q_ref,
                 ang_ref, idx_ref, s_ref, out_pay, sib_pay,
                 in_sem, w_sem, k_sem, v_sem, send_sem, recv_sem):
    n_seq, d_model = h_ref.shape
    rows = k_ref.shape[1]
    head = k_ref.shape[2]
    w_chunks, _, w_cols = w_buf.shape
    n_q = q_ref.shape[1]
    kv_local = n_q // 4
    sp = lax.axis_index('sp')
    core = sp % 2
    sib = {'sp': sp + 1 - 2 * core}
    base = sp * (rows // kv_local)
    starts = quarters(n_seq)
    q4 = n_seq // 4
    per_slot = q4 // PART

    small = [pltpu.make_async_copy(h_hbm, h_ref, in_sem.at[0]),
             pltpu.make_async_copy(scale_hbm, scale_ref, in_sem.at[1]),
             pltpu.make_async_copy(pos_hbm, pos_ref, in_sem.at[2])]
    for cp in small:
        cp.start()

    def w_copy(t):
        at = pl.multiple_of((core * w_chunks + t) * w_cols, 128)
        return pltpu.make_async_copy(w_ref.at[:, pl.ds(at, w_cols)], w_buf.at[t], w_sem.at[t])

    def c_copies(i):
        src = pl.ds(starts[i // per_slot] + (i % per_slot) * PART, PART)
        dst = pl.ds(i * PART, PART)
        return (pltpu.make_async_copy(kc_ref.at[src], k_ref.at[dst], k_sem.at[i]),
                pltpu.make_async_copy(vc_ref.at[src], v_ref.at[dst], v_sem.at[i]))

    for t in range(w_chunks):
        w_copy(t).start()

    barrier = pltpu.get_barrier_semaphore()
    pl.semaphore_signal(barrier, inc=1, device_id=sib, device_id_type=MESH)

    idx_ref[...] = row_index(n_q, rows)

    lane = lax.broadcasted_iota(jnp.int32, (1, head), 1)
    half = head // 2
    inv_freq = jnp.exp((lane % half).astype(jnp.float32) * (-2.0 * math.log(500000.0) / head))
    small[2].wait()

    def fill(b, _):
        ang_ref[pl.ds(b, 1), :] = jnp.full((1, head), pos_ref[b].astype(jnp.float32)) * inv_freq
        return 0
    lax.fori_loop(0, n_seq, fill, 0)
    cos = jnp.cos(ang_ref[...])
    sin = jnp.sin(ang_ref[...]) * jnp.where(lane < half, -1.0, 1.0)

    def rope(x):
        return (x * cos + pltpu.roll(x, half, 1) * sin).astype(jnp.bfloat16).astype(jnp.float32)

    small[0].wait()
    small[1].wait()
    blocks = d_model // 128
    total = jnp.zeros((n_seq, 128), jnp.float32)
    for i in range(blocks):
        total += h_ref[:, i * 128:(i + 1) * 128].astype(jnp.float32)
    mean = jnp.sum(total, axis=1, keepdims=True) * (1.0 / d_model)
    total = jnp.zeros((n_seq, 128), jnp.float32)
    for i in range(blocks):
        cen = h_ref[:, i * 128:(i + 1) * 128].astype(jnp.float32) - mean
        total += cen * cen
    var = jnp.sum(total, axis=1, keepdims=True) * (1.0 / d_model)
    rstd = lax.rsqrt(var + LN_EPS)
    for i in range(blocks):
        cen = h_ref[:, i * 128:(i + 1) * 128].astype(jnp.float32) - mean
        u_ref[:, i * 128:(i + 1) * 128] = (
            cen * rstd * scale_ref[i:i + 1, :].astype(jnp.float32)).astype(jnp.bfloat16)
    pl.semaphore_wait(barrier, 1)

    heads = w_cols // head
    sends = []
    for t in range(w_chunks):
        w_copy(t).wait()
        if t == 0:
            for i in range(4 * per_slot):
                for c in c_copies(i):
                    c.start(priority=1)
        acc = jnp.dot(u_ref[...], w_buf[t], preferred_element_type=jnp.float32)
        qkv = jnp.clip(acc.astype(jnp.bfloat16).astype(jnp.float32), -8.0, 8.0)
        at = (core * w_chunks + t) * heads
        for j in range(heads):
            val = qkv[:, j * head:(j + 1) * head]
            qkv_ref[at + j] = rope(val) if (t * heads + j) % 6 < 5 else val
        block = qkv_ref.at[pl.ds(at, heads)]
        sends.append(pltpu.make_async_remote_copy(
            src_ref=block, dst_ref=block, send_sem=send_sem.at[t], recv_sem=recv_sem.at[t],
            device_id=sib, device_id_type=MESH))
        sends[t].start()
    for cp in sends:
        cp.wait_recv()
    for g in range(kv_local):
        for j in range(4):
            q_ref[:, g * 4 + j, :] = qkv_ref[g * 6 + j]

    lane_id = lax.broadcasted_iota(jnp.int32, (n_q, 128), 1)
    pays = [out_pay, pay_ref]
    stats = [jnp.zeros((n_q, 128), jnp.float32) for _ in pays]
    pay_copy = pltpu.make_async_remote_copy(
        src_ref=out_pay, dst_ref=sib_pay, send_sem=send_sem.at[w_chunks], recv_sem=recv_sem.at[w_chunks],
        device_id=sib, device_id_type=MESH)

    def seq(b):
        return starts[b // q4] + b % q4

    def arrive(i):
        for c in c_copies(i):
            c.wait()

    def out_at(b, o, m, l):
        if b < 2 * kv_local:
            g, new_ref = b // 2, (kn_ref, vn_ref)[b % 2]
            for r in range(16 // kv_local):
                new_ref[:, r * kv_local + g, :] = qkv_ref[g * 6 + 4 + b % 2]
        slot = b // q4
        pays[slot][b % q4] = o
        stats[slot] = put_stats(stats[slot], lane_id, b % q4, m, l)
        if b == q4 - 1:
            out_pay[q4] = stats[0]
            pay_copy.start()

    parts = [list(range(i * PART, (i + 1) * PART)) for i in range(2 * per_slot)]
    attend_parts(parts, arrive, lambda b: q_ref[seq(b)], lambda b: pos_ref[seq(b)] - base - 1,
                 k_ref, v_ref, idx_ref, s_ref, out_at)

    pay_copy.wait_recv()
    other = sib_pay[q4]
    top = jnp.maximum(stats[1], other)
    f0, f1 = jnp.exp(stats[1] - top), jnp.exp(other - top)
    total = pltpu.roll(stats[1], 64, 1) * f0 + pltpu.roll(other, 64, 1) * f1
    pay_ref[q4] = jnp.where(lane_id < 64, top, pltpu.roll(total, 64, 1))
    for i in range(q4):
        pay_ref[i] = (pay_ref[i] * jnp.broadcast_to(f0[:, i:i + 1], (n_q, 128))
                      + sib_pay[i] * jnp.broadcast_to(f1[:, i:i + 1], (n_q, 128)))
    q_own[...] = q_ref[pl.ds(starts[2], 2 * q4)]
    for i in range(2 * per_slot, 4 * per_slot):
        arrive(i)
    for cp in sends + [pay_copy]:
        cp.wait_send()


def second_kernel(pos_hbm, q_ref, kn_ref, vn_ref, k_ref, v_ref,
                  ko_ref, vo_ref, pay_ref, k_late, v_late,
                  pos_ref, idx_ref, s_ref,
                  in_sem, o_sem):
    n_seq, rows, head = k_ref.shape
    half_seq, n_q = q_ref.shape[:2]
    kv_local = n_q // 4
    sp = lax.axis_index('sp')
    core = sp % 2
    base = sp * (rows // kv_local)
    starts = quarters(n_seq)
    q4 = n_seq // 4

    pos_copy = pltpu.make_async_copy(pos_hbm, pos_ref, in_sem.at[0])
    pos_copy.start()
    idx_ref[...] = row_index(n_q, rows)
    pos_copy.wait()

    for i in range(EARLY_PARTS):
        insert_part(i, starts, base, pos_ref, k_ref, v_ref, kn_ref, vn_ref)
        for c in write_copies(i, starts, q4, k_ref, v_ref, ko_ref, vo_ref, o_sem):
            c.start()

    late = EARLY_PARTS * PART

    def late_row(k):
        k_late[k - late] = k_ref[k]
        v_late[k - late] = v_ref[k]
        b = starts[k // q4] + k % q4
        insert_row(k_late, v_late, k - late, pos_ref[b] - base, kn_ref[b], vn_ref[b])

    lane_id = lax.broadcasted_iota(jnp.int32, (n_q, 128), 1)
    stats = [jnp.zeros((n_q, 128), jnp.float32)]

    def per_head(tile):
        return jnp.concatenate([jnp.broadcast_to(tile[g:g + 1], (4, head)) for g in range(kv_local)], axis=0)

    def out_at(b, o, m, l):
        k = b - half_seq
        at = starts[2] + k
        s = jnp.sum(q_ref[k] * per_head(kn_ref[at]), axis=1, keepdims=True) * head ** -0.5
        s = jnp.where(core == k // q4, s, NEG)
        top = jnp.maximum(m, s)
        old = jnp.exp(m - top)
        new = jnp.where(core == k // q4, jnp.exp(s - top), 0.0)
        pay_ref[k] = o * old + new.astype(jnp.bfloat16).astype(jnp.float32) * per_head(vn_ref[at])
        stats[0] = put_stats(stats[0], lane_id, k, top, l * old + new)
        if b >= late:
            late_row(b)

    parts = [list(range(half_seq + i, half_seq + i + PART)) for i in range(0, half_seq, PART)]
    attend_parts(parts, lambda i: None, lambda b: q_ref[b - half_seq],
                 lambda b: pos_ref[starts[2] + b - half_seq] - base - 1,
                 k_ref, v_ref, idx_ref, s_ref, out_at)
    pay_ref[half_seq] = stats[0]
    for i in range(EARLY_PARTS):
        for c in write_copies(i, starts, q4, k_ref, v_ref, ko_ref, vo_ref, o_sem):
            c.wait()


def third_kernel(k_late, v_late, k_in, v_in, ko_ref, vo_ref, o_sem):
    n_seq = ko_ref.shape[0]
    starts = quarters(n_seq)
    parts = range(EARLY_PARTS, n_seq // PART)
    for i in parts:
        for c in write_copies(i, starts, n_seq // 4, k_late, v_late, ko_ref, vo_ref, o_sem, EARLY_PARTS):
            c.start()
    for i in parts:
        for c in write_copies(i, starts, n_seq // 4, k_late, v_late, ko_ref, vo_ref, o_sem, EARLY_PARTS):
            c.wait()


def finish_kernel(h_ref, w_ref, mine_ref, sib_ref, got_ref, sib_got_ref, out_ref,
                  w_buf, att, got2, lhs, part, y_in, fin, x_in, d_in, d_in2,
                  w_sem, ys_sem, yr_sem, xs_sem, xr_sem, ds_sem, dr_sem, es_sem, er_sem):
    n_q = mine_ref.shape[1]
    sp = lax.axis_index('sp')
    tp = lax.axis_index('tp')
    x, c = sp // 2, sp % 2
    sib = {'sp': x * 2 + (1 - c)}
    xn = {'sp': (1 - x) * 2 + c}
    yn = {'tp': 1 - tp}

    half_cols = w_buf.shape[1]
    cc = half_cols // OUT_CHUNKS
    q4 = got_ref.shape[0] - 1
    own_col = c * half_cols
    oth_col = (1 - c) * half_cols

    def w_copy(j):
        return pltpu.make_async_copy(
            w_ref.at[:, pl.ds(pl.multiple_of(own_col + j * cc, 128), cc)],
            w_buf.at[:, pl.ds(j * cc, cc)], w_sem.at[j])

    for j in range(OUT_CHUNKS):
        w_copy(j).start()

    barrier = pltpu.get_barrier_semaphore()
    for dev in (sib, xn, yn):
        pl.semaphore_signal(barrier, inc=1, device_id=dev, device_id_type=MESH)

    def remote(src, dst, ssem, rsem, dev):
        return pltpu.make_async_remote_copy(src_ref=src, dst_ref=dst, send_sem=ssem, recv_sem=rsem,
                                            device_id=dev, device_id_type=MESH)

    got2[c] = got_ref[...]
    got2[1 - c] = sib_got_ref[...]

    lane_id = lax.broadcasted_iota(jnp.int32, (n_q, 128), 1)
    far = got2[1, q4]
    far = jnp.where(lane_id % 64 < q4, got2[0, q4], pltpu.roll(far, q4, 1))
    maxes = [mine_ref[2 * q4], sib_ref[2 * q4], far]
    sums = [pltpu.roll(m, 64, 1) for m in maxes]
    top = jnp.maximum(jnp.maximum(maxes[0], maxes[1]), maxes[2])
    factors = [jnp.exp(m - top) for m in maxes]
    inv = 1.0 / (sums[0] * factors[0] + sums[1] * factors[1] + sums[2] * factors[2])
    factors = [f * inv for f in factors]
    for i in range(2 * q4):
        f0, f1, f2 = (jnp.broadcast_to(f[:, i:i + 1], (n_q, 128)) for f in factors)
        att[i] = mine_ref[i] * f0 + sib_ref[i] * f1 + got2[i // q4, i % q4] * f2
    for n in range(n_q):
        lhs[:, n * 128:(n + 1) * 128] = att[:, n, :].astype(jnp.bfloat16)

    y_copy, x_copy, d_copy, e_copy = [], [], [], []
    for j in range(OUT_CHUNKS):
        w_copy(j).wait()
        part[j] = jnp.dot(lhs[...], w_buf[:, j * cc:(j + 1) * cc], preferred_element_type=jnp.float32)
        if j == 0:
            pl.semaphore_wait(barrier, 3)
        y_copy.append(remote(part.at[j], y_in.at[j], ys_sem.at[j], yr_sem.at[j], yn))
        y_copy[j].start()

    my_rows = pl.ds(pl.multiple_of(x * (2 * q4), 2 * q4), 2 * q4)
    xn_rows = pl.ds(pl.multiple_of((1 - x) * (2 * q4), 2 * q4), 2 * q4)

    def cols(start, j):
        return pl.ds(pl.multiple_of(start + j * cc, 128), cc)

    for j in range(OUT_CHUNKS):
        y_copy[j].wait_recv()
        fin[j] = h_ref[my_rows, cols(own_col, j)].astype(jnp.float32) + (part[j] + y_in[j])
        x_copy.append(remote(fin.at[j], x_in.at[j], xs_sem.at[j], xr_sem.at[j], xn))
        x_copy[j].start()
        d_copy.append(remote(fin.at[j], d_in.at[j], ds_sem.at[j], dr_sem.at[j], sib))
        d_copy[j].start()
        out_ref[my_rows, cols(own_col, j)] = fin[j].astype(jnp.bfloat16)
    for j in range(OUT_CHUNKS):
        x_copy[j].wait_recv()
        e_copy.append(remote(x_in.at[j], d_in2.at[j], es_sem.at[j], er_sem.at[j], sib))
        e_copy[j].start()
        out_ref[xn_rows, cols(own_col, j)] = x_in[j].astype(jnp.bfloat16)
        d_copy[j].wait_recv()
        out_ref[my_rows, cols(oth_col, j)] = d_in[j].astype(jnp.bfloat16)
    for j in range(OUT_CHUNKS):
        e_copy[j].wait_recv()
        out_ref[xn_rows, cols(oth_col, j)] = d_in2[j].astype(jnp.bfloat16)

    for cp in y_copy + x_copy + d_copy + e_copy:
        cp.wait_send()


def solution(mesh):
    cache_spec = P('dp', 'sp', 'tp', None)

    def local_step(hidden, norm_scale, w_qkv, w_out, k_cache, v_cache, positions):
        n_seq, seq_local, kv_local, head = k_cache.shape
        d_model = hidden.shape[1]
        rows = seq_local * kv_local
        n_q = 4 * kv_local
        q4 = n_seq // 4
        vm = pl.BlockSpec(memory_space=pltpu.VMEM)
        hbm = pl.BlockSpec(memory_space=pltpu.HBM)
        dma = pltpu.SemaphoreType.DMA
        f32, bf16 = jnp.float32, jnp.bfloat16
        payload = pltpu.VMEM((q4 + 1, n_q, head), f32)
        payload2 = pltpu.VMEM((2 * q4 + 1, n_q, head), f32)
        k_rows = k_cache.reshape(n_seq, rows, head)
        v_rows = v_cache.reshape(n_seq, rows, head)
        slots = n_seq // PART
        late = pltpu.VMEM((n_seq - EARLY_PARTS * PART, rows, head), bf16)
        w_chunks = 3 * kv_local // W_HEADS

        def pin(a):
            return pltpu.with_memory_space_constraint(a, pltpu.HBM)

        k_all, v_all, pay, q_own, kn, vn = pl.pallas_call(
            first_kernel,
            out_shape=(pltpu.VMEM((n_seq, rows, head), bf16), pltpu.VMEM((n_seq, rows, head), bf16),
                       payload,
                       pltpu.VMEM((2 * q4, n_q, head), f32), pltpu.VMEM((n_seq, 16, head), f32),
                       pltpu.VMEM((n_seq, 16, head), f32)),
            in_specs=[hbm] * 6,
            out_specs=(vm,) * 6,
            scratch_shapes=[
                pltpu.SMEM((n_seq,), jnp.int32),
                pltpu.VMEM((n_seq, d_model), bf16),
                pltpu.VMEM((d_model // 128, 128), bf16),
                pltpu.VMEM((w_chunks, d_model, W_HEADS * head), bf16),
                pltpu.VMEM((n_seq, d_model), bf16),
                pltpu.VMEM((6 * kv_local, n_seq, head), f32),
                pltpu.VMEM((n_seq, n_q, head), f32),
                pltpu.VMEM((n_seq, head), f32),
                pltpu.VMEM((n_q, rows), jnp.int32),
                pltpu.VMEM((2, PART, n_q, rows), f32),
                payload, payload,
                dma((3,)), dma((w_chunks,)), dma((slots,)), dma((slots,)),
                dma((w_chunks + 1,)), dma((w_chunks + 1,)),
            ],
            compiler_params=pltpu.CompilerParams(
                collective_id=1, has_side_effects=True, vmem_limit_bytes=FIRST_VMEM * 1024 * 1024),
            cost_estimate=pl.CostEstimate(flops=2 * 10**10, bytes_accessed=4 * 10**7, transcendentals=0),
            name='first',
        )(*map(pin, (positions, hidden, norm_scale.reshape(d_model // 128, 128), w_qkv, k_rows, v_rows)))

        got = lax.ppermute(pay, 'sp', [(i, i ^ 2) for i in range(4)])

        k_part, v_part, mine, k_late, v_late = pl.pallas_call(
            second_kernel,
            out_shape=(jax.ShapeDtypeStruct((n_seq, rows, head), bf16),
                       jax.ShapeDtypeStruct((n_seq, rows, head), bf16), payload2, late, late),
            in_specs=[hbm, vm, vm, vm, vm, vm],
            out_specs=(hbm, hbm, vm, vm, vm),
            scratch_shapes=[
                pltpu.SMEM((n_seq,), jnp.int32),
                pltpu.VMEM((n_q, rows), jnp.int32),
                pltpu.VMEM((2, PART, n_q, rows), f32),
                dma((1,)), dma((2, n_seq // PART)),
            ],
            compiler_params=pltpu.CompilerParams(vmem_limit_bytes=12 * 1024 * 1024),
            cost_estimate=pl.CostEstimate(flops=2 * 10**10, bytes_accessed=4 * 10**7, transcendentals=0),
            name='second',
        )(positions, q_own, kn, vn, k_all, v_all)

        swap = [(i, i ^ 1) for i in range(4)]
        sib_mine = lax.ppermute(mine, 'sp', swap)
        sib_got = lax.ppermute(got, 'sp', swap)

        k_upd, v_upd = pl.pallas_call(
            third_kernel,
            out_shape=(jax.ShapeDtypeStruct((n_seq, rows, head), bf16),
                       jax.ShapeDtypeStruct((n_seq, rows, head), bf16)),
            in_specs=[vm, vm, hbm, hbm],
            out_specs=(hbm, hbm),
            input_output_aliases={2: 0, 3: 1},
            scratch_shapes=[dma((2, n_seq // PART))],
            compiler_params=pltpu.CompilerParams(vmem_limit_bytes=12 * 1024 * 1024),
            cost_estimate=pl.CostEstimate(flops=2 * 10**10, bytes_accessed=4 * 10**7, transcendentals=0),
            name='third',
        )(k_late, v_late, k_part, v_part)

        half_cols = d_model // 2
        cc = half_cols // OUT_CHUNKS
        chunk = pltpu.VMEM((OUT_CHUNKS, 2 * q4, cc), f32)
        h_out = pl.pallas_call(
            finish_kernel,
            out_shape=jax.ShapeDtypeStruct((n_seq, d_model), bf16),
            in_specs=[vm, hbm, vm, vm, vm, vm],
            out_specs=vm,
            scratch_shapes=[
                pltpu.VMEM((w_out.shape[0], half_cols), bf16),
                pltpu.VMEM((2 * q4, n_q, head), f32),
                pltpu.VMEM((2, q4 + 1, n_q, head), f32),
                pltpu.VMEM((2 * q4, n_q * head), bf16),
                chunk, chunk, chunk, chunk, chunk, chunk,
                dma((OUT_CHUNKS,)),
                dma((OUT_CHUNKS,)), dma((OUT_CHUNKS,)),
                dma((OUT_CHUNKS,)), dma((OUT_CHUNKS,)),
                dma((OUT_CHUNKS,)), dma((OUT_CHUNKS,)),
                dma((OUT_CHUNKS,)), dma((OUT_CHUNKS,)),
            ],
            compiler_params=pltpu.CompilerParams(
                collective_id=0, has_side_effects=True, vmem_limit_bytes=50 * 1024 * 1024),
            name='finish',
        )(hidden, pin(w_out), mine, sib_mine, got, sib_got)
        return h_out, k_upd.reshape(k_cache.shape), v_upd.reshape(v_cache.shape)

    return jax.shard_map(
        local_step,
        mesh=mesh,
        in_specs=(P('dp', None), P(None), P(None, 'tp'), P('tp', None), cache_spec, cache_spec, P('dp')),
        out_specs=(P('dp', None), cache_spec, cache_spec),
        check_vma=False,
    )
```

```python
import math

import jax
import jax.numpy as jnp
from jax import lax
from jax.experimental import pallas as pl
from jax.experimental.pallas import tpu as pltpu
from jax.sharding import PartitionSpec as P

MESH = pl.DeviceIdType.MESH
NEG = -1e30
PV_LAG = 8
W_SPLIT = (4, 4, 4)
PART = 8
EARLY_PARTS = 7
DOTS = 8
OUT_CHUNKS = 8
LN_EPS = 1e-5
FIRST_VMEM = 36


def quarters(n_seq):
    sp = lax.axis_index('sp')
    x, c = sp // 2, sp % 2
    q = n_seq // 4

    def start(xx, cc):
        return pl.multiple_of((xx * 2 + cc) * q, q)
    own = start(x, 0)
    return [start(1 - x, 1 - c), start(1 - x, c), own, pl.multiple_of(own + q, q)]


def insert_row(k_ref, v_ref, at_b, p, kn, vn):
    rows, head = k_ref.shape[1:]
    kv_local = rows // 128
    per = 16 // kv_local
    tile = jnp.clip(p // per, 0, rows // 16 - 1)
    at = pl.ds(pl.multiple_of(tile * 16, 16), 16)
    hit = lax.broadcasted_iota(jnp.int32, (16, head), 0) // kv_local == p - tile * per
    kn, vn = (jnp.concatenate([new[:kv_local]] * per, axis=0) for new in (kn, vn))
    k_ref[at_b, at, :] = jnp.where(hit, kn, k_ref[at_b, at, :].astype(jnp.float32)).astype(jnp.bfloat16)
    v_ref[at_b, at, :] = jnp.where(hit, vn, v_ref[at_b, at, :].astype(jnp.float32)).astype(jnp.bfloat16)


def write_copies(i, starts, q4, k_ref, v_ref, ko_ref, vo_ref, sem, first=0):
    at = i * PART
    src = pl.ds(at - first * PART, PART)
    dst = pl.ds(starts[at // q4] + at % q4, PART)
    return (pltpu.make_async_copy(k_ref.at[src], ko_ref.at[dst], sem.at[0, i]),
            pltpu.make_async_copy(v_ref.at[src], vo_ref.at[dst], sem.at[1, i]))


def insert_part(i, starts, base, pos_ref, k_ref, v_ref, kn_ref, vn_ref):
    q4 = k_ref.shape[0] // 4
    for k in range(i * PART, (i + 1) * PART):
        b = starts[k // q4] + k % q4
        insert_row(k_ref, v_ref, k, pos_ref[b] - base, kn_ref[b], vn_ref[b])


def row_index(n_q, rows):
    kv_local = n_q // 4
    col = lax.broadcasted_iota(jnp.int32, (n_q, rows), 1)
    qg = lax.broadcasted_iota(jnp.int32, (n_q, rows), 0) // 4
    return jnp.where(col % kv_local == qg, col // kv_local, 1 << 20)


def attend_parts(parts, arrive, q_at, p_at, k_ref, v_ref, idx_ref, s_ref, out_at):
    scale = k_ref.shape[2] ** -0.5

    def scores(b, slot, k):
        s_ref[slot, k] = lax.dot_general(
            q_at(b).astype(jnp.bfloat16), k_ref[b], (((1,), (1,)), ((), ())),
            preferred_element_type=jnp.float32)

    arrive(0)
    for k, b in enumerate(parts[0]):
        scores(b, 0, k)
    for i, part in enumerate(parts):
        more = i + 1 < len(parts)
        if more:
            arrive(i + 1)
        held = [None] * len(part)
        for k in range(len(part) + PV_LAG):
            if k < len(part):
                if more:
                    scores(parts[i + 1][k], (i + 1) % 2, k)
                s = jnp.where(idx_ref[...] <= p_at(part[k]), s_ref[i % 2, k] * scale, NEG)
                m = jnp.max(s, axis=1, keepdims=True)
                e = jnp.exp(s - m)
                held[k] = (e.astype(jnp.bfloat16), m, jnp.sum(e, axis=1, keepdims=True))
            if k >= PV_LAG:
                b = part[k - PV_LAG]
                e, m, l = held[k - PV_LAG]
                out_at(b, jnp.dot(e, v_ref[b], preferred_element_type=jnp.float32), m, l)


def put_stats(tile, lane_id, k, m, l):
    return jnp.where(lane_id == k, m, jnp.where(lane_id == 64 + k, l, tile))


def first_kernel(pos_hbm, h_hbm, scale_hbm, w_ref, kc_ref, vc_ref,
                 k_ref, v_ref, pay_ref, q_own, kn_ref, vn_ref,
                 pos_ref, h_ref, scale_ref, w_buf, u_ref, qkv_ref, q_ref,
                 ang_ref, idx_ref, s_ref, out_pay, sib_pay,
                 in_sem, w_sem, k_sem, v_sem, send_sem, recv_sem):
    n_seq, d_model = h_ref.shape
    rows = k_ref.shape[1]
    head = k_ref.shape[2]
    w_chunks = len(W_SPLIT)
    half_heads = w_buf.shape[1] // head
    first_head = [sum(W_SPLIT[:t]) for t in range(w_chunks + 1)]
    n_q = q_ref.shape[1]
    kv_local = n_q // 4
    sp = lax.axis_index('sp')
    core = sp % 2
    sib = {'sp': sp + 1 - 2 * core}
    base = sp * (rows // kv_local)
    starts = quarters(n_seq)
    q4 = n_seq // 4
    per_slot = q4 // PART

    small = [pltpu.make_async_copy(h_hbm, h_ref, in_sem.at[0]),
             pltpu.make_async_copy(scale_hbm, scale_ref, in_sem.at[1]),
             pltpu.make_async_copy(pos_hbm, pos_ref, in_sem.at[2])]
    for cp in small:
        cp.start()

    def w_copy(t):
        at, width = first_head[t] * head, W_SPLIT[t] * head
        src = pl.ds(pl.multiple_of(core * half_heads * head + at, 128), width)
        return pltpu.make_async_copy(w_ref.at[:, src], w_buf.at[:, pl.ds(at, width)], w_sem.at[t])

    def c_copies(i):
        src = pl.ds(starts[i // per_slot] + (i % per_slot) * PART, PART)
        dst = pl.ds(i * PART, PART)
        return (pltpu.make_async_copy(kc_ref.at[src], k_ref.at[dst], k_sem.at[i]),
                pltpu.make_async_copy(vc_ref.at[src], v_ref.at[dst], v_sem.at[i]))

    for t in range(w_chunks):
        w_copy(t).start()

    barrier = pltpu.get_barrier_semaphore()
    pl.semaphore_signal(barrier, inc=1, device_id=sib, device_id_type=MESH)

    idx_ref[...] = row_index(n_q, rows)

    lane = lax.broadcasted_iota(jnp.int32, (1, head), 1)
    half = head // 2
    inv_freq = jnp.exp((lane % half).astype(jnp.float32) * (-2.0 * math.log(500000.0) / head))
    small[2].wait()

    def fill(b, _):
        ang_ref[pl.ds(b, 1), :] = jnp.full((1, head), pos_ref[b].astype(jnp.float32)) * inv_freq
        return 0
    lax.fori_loop(0, n_seq, fill, 0)
    cos = jnp.cos(ang_ref[...])
    sin = jnp.sin(ang_ref[...]) * jnp.where(lane < half, -1.0, 1.0)

    def rope(x):
        return (x * cos + pltpu.roll(x, half, 1) * sin).astype(jnp.bfloat16).astype(jnp.float32)

    small[0].wait()
    small[1].wait()
    blocks = d_model // 128
    total = jnp.zeros((n_seq, 128), jnp.float32)
    for i in range(blocks):
        total += h_ref[:, i * 128:(i + 1) * 128].astype(jnp.float32)
    mean = jnp.sum(total, axis=1, keepdims=True) * (1.0 / d_model)
    total = jnp.zeros((n_seq, 128), jnp.float32)
    for i in range(blocks):
        cen = h_ref[:, i * 128:(i + 1) * 128].astype(jnp.float32) - mean
        total += cen * cen
    var = jnp.sum(total, axis=1, keepdims=True) * (1.0 / d_model)
    rstd = lax.rsqrt(var + LN_EPS)
    for i in range(blocks):
        cen = h_ref[:, i * 128:(i + 1) * 128].astype(jnp.float32) - mean
        u_ref[:, i * 128:(i + 1) * 128] = (
            cen * rstd * scale_ref[i:i + 1, :].astype(jnp.float32)).astype(jnp.bfloat16)
    pl.semaphore_wait(barrier, 1)

    sends = []
    for t in range(w_chunks):
        w_copy(t).wait()
        if t == 0:
            for i in range(4 * per_slot):
                for c in c_copies(i):
                    c.start(priority=1)
        acc = jnp.dot(u_ref[...], w_buf[:, first_head[t] * head:first_head[t + 1] * head],
                      preferred_element_type=jnp.float32)
        qkv = jnp.clip(acc.astype(jnp.bfloat16).astype(jnp.float32), -8.0, 8.0)
        at = core * half_heads + first_head[t]
        for j in range(W_SPLIT[t]):
            val = qkv[:, j * head:(j + 1) * head]
            qkv_ref[at + j] = rope(val) if (first_head[t] + j) % 6 < 5 else val
        block = qkv_ref.at[pl.ds(at, W_SPLIT[t])]
        sends.append(pltpu.make_async_remote_copy(
            src_ref=block, dst_ref=block, send_sem=send_sem.at[t], recv_sem=recv_sem.at[t],
            device_id=sib, device_id_type=MESH))
        sends[t].start()
    for cp in sends:
        cp.wait_recv()
    half_seq = n_seq // 2
    far_half = pl.ds(pl.multiple_of(half_seq - starts[2], half_seq), half_seq)
    own_half = pl.ds(starts[2], half_seq)
    for g in range(kv_local):
        for j in range(4):
            q_ref[:, g * 4 + j, :] = qkv_ref[g * 6 + j, far_half]

    lane_id = lax.broadcasted_iota(jnp.int32, (n_q, 128), 1)
    pays = [out_pay, pay_ref]
    stats = [jnp.zeros((n_q, 128), jnp.float32) for _ in pays]
    pay_copy = pltpu.make_async_remote_copy(
        src_ref=out_pay, dst_ref=sib_pay, send_sem=send_sem.at[w_chunks], recv_sem=recv_sem.at[w_chunks],
        device_id=sib, device_id_type=MESH)

    def seq(b):
        return starts[b // q4] + b % q4

    def arrive(i):
        for c in c_copies(i):
            c.wait()

    def out_at(b, o, m, l):
        if b < 6 * kv_local:
            g, kind = divmod(b, 6)
            if kind < 4:
                q_own[:, g * 4 + kind, :] = qkv_ref[b, own_half]
            else:
                (kn_ref, vn_ref)[kind - 4][:, g, :] = qkv_ref[b]
        slot = b // q4
        pays[slot][b % q4] = o
        stats[slot] = put_stats(stats[slot], lane_id, b % q4, m, l)
        if b == q4 - 1:
            out_pay[q4] = stats[0]
            pay_copy.start()

    parts = [list(range(i * PART, (i + 1) * PART)) for i in range(2 * per_slot)]
    attend_parts(parts, arrive, lambda b: q_ref[seq(b) - half_seq + starts[2]], lambda b: pos_ref[seq(b)] - base - 1,
                 k_ref, v_ref, idx_ref, s_ref, out_at)

    pay_copy.wait_recv()
    other = sib_pay[q4]
    top = jnp.maximum(stats[1], other)
    f0, f1 = jnp.exp(stats[1] - top), jnp.exp(other - top)
    total = pltpu.roll(stats[1], 64, 1) * f0 + pltpu.roll(other, 64, 1) * f1
    pay_ref[q4] = jnp.where(lane_id < 64, top, pltpu.roll(total, 64, 1))
    for i in range(q4):
        pay_ref[i] = (pay_ref[i] * jnp.broadcast_to(f0[:, i:i + 1], (n_q, 128))
                      + sib_pay[i] * jnp.broadcast_to(f1[:, i:i + 1], (n_q, 128)))
    for i in range(2 * per_slot, 4 * per_slot):
        arrive(i)
    for cp in sends + [pay_copy]:
        cp.wait_send()


def second_kernel(pos_hbm, q_ref, kn_ref, vn_ref, k_ref, v_ref,
                  ko_ref, vo_ref, pay_ref, k_late, v_late,
                  pos_ref, idx_ref, s_ref,
                  in_sem, o_sem):
    n_seq, rows, head = k_ref.shape
    half_seq, n_q = q_ref.shape[:2]
    kv_local = n_q // 4
    sp = lax.axis_index('sp')
    core = sp % 2
    base = sp * (rows // kv_local)
    starts = quarters(n_seq)
    q4 = n_seq // 4

    pos_copy = pltpu.make_async_copy(pos_hbm, pos_ref, in_sem.at[0])
    pos_copy.start()
    idx_ref[...] = row_index(n_q, rows)
    pos_copy.wait()

    for i in range(EARLY_PARTS):
        insert_part(i, starts, base, pos_ref, k_ref, v_ref, kn_ref, vn_ref)
        for c in write_copies(i, starts, q4, k_ref, v_ref, ko_ref, vo_ref, o_sem):
            c.start()

    late = EARLY_PARTS * PART

    def late_row(k):
        k_late[k - late] = k_ref[k]
        v_late[k - late] = v_ref[k]
        b = starts[k // q4] + k % q4
        insert_row(k_late, v_late, k - late, pos_ref[b] - base, kn_ref[b], vn_ref[b])

    lane_id = lax.broadcasted_iota(jnp.int32, (n_q, 128), 1)
    stats = [jnp.zeros((n_q, 128), jnp.float32)]

    def per_head(tile):
        return jnp.concatenate([jnp.broadcast_to(tile[g:g + 1], (4, head)) for g in range(kv_local)], axis=0)

    def out_at(b, o, m, l):
        k = b - half_seq
        at = starts[2] + k
        s = jnp.sum(q_ref[k] * per_head(kn_ref[at]), axis=1, keepdims=True) * head ** -0.5
        s = jnp.where(core == k // q4, s, NEG)
        top = jnp.maximum(m, s)
        old = jnp.exp(m - top)
        new = jnp.where(core == k // q4, jnp.exp(s - top), 0.0)
        pay_ref[k] = o * old + new.astype(jnp.bfloat16).astype(jnp.float32) * per_head(vn_ref[at])
        stats[0] = put_stats(stats[0], lane_id, k, top, l * old + new)
        if b >= late:
            late_row(b)

    parts = [list(range(half_seq + i, half_seq + i + PART)) for i in range(0, half_seq, PART)]
    attend_parts(parts, lambda i: None, lambda b: q_ref[b - half_seq],
                 lambda b: pos_ref[starts[2] + b - half_seq] - base - 1,
                 k_ref, v_ref, idx_ref, s_ref, out_at)
    pay_ref[half_seq] = stats[0]
    for i in range(EARLY_PARTS):
        for c in write_copies(i, starts, q4, k_ref, v_ref, ko_ref, vo_ref, o_sem):
            c.wait()


def third_kernel(k_late, v_late, k_in, v_in, ko_ref, vo_ref, o_sem):
    n_seq = ko_ref.shape[0]
    starts = quarters(n_seq)
    parts = range(EARLY_PARTS, n_seq // PART)
    for i in parts:
        for c in write_copies(i, starts, n_seq // 4, k_late, v_late, ko_ref, vo_ref, o_sem, EARLY_PARTS):
            c.start()
    for i in parts:
        for c in write_copies(i, starts, n_seq // 4, k_late, v_late, ko_ref, vo_ref, o_sem, EARLY_PARTS):
            c.wait()


def finish_kernel(h_ref, w_ref, mine_ref, sib_ref, got_ref, sib_got_ref, out_ref,
                  w_buf, att, got2, lhs, part, y_in, fin, x_in, d_in, d_in2,
                  w_sem, ys_sem, yr_sem, xs_sem, xr_sem, ds_sem, dr_sem, es_sem, er_sem):
    n_q = mine_ref.shape[1]
    sp = lax.axis_index('sp')
    tp = lax.axis_index('tp')
    x, c = sp // 2, sp % 2
    sib = {'sp': x * 2 + (1 - c)}
    xn = {'sp': (1 - x) * 2 + c}
    yn = {'tp': 1 - tp}

    half_cols = w_buf.shape[1]
    cc = half_cols // OUT_CHUNKS
    q4 = got_ref.shape[0] - 1
    own_col = c * half_cols
    oth_col = (1 - c) * half_cols

    wc = half_cols // DOTS
    per_dot = OUT_CHUNKS // DOTS

    def w_copy(j):
        return pltpu.make_async_copy(
            w_ref.at[:, pl.ds(pl.multiple_of(own_col + j * wc, 128), wc)],
            w_buf.at[:, pl.ds(j * wc, wc)], w_sem.at[j])

    for j in range(DOTS):
        w_copy(j).start()

    barrier = pltpu.get_barrier_semaphore()
    for dev in (sib, xn, yn):
        pl.semaphore_signal(barrier, inc=1, device_id=dev, device_id_type=MESH)

    def remote(src, dst, ssem, rsem, dev):
        return pltpu.make_async_remote_copy(src_ref=src, dst_ref=dst, send_sem=ssem, recv_sem=rsem,
                                            device_id=dev, device_id_type=MESH)

    got2[c] = got_ref[...]
    got2[1 - c] = sib_got_ref[...]

    lane_id = lax.broadcasted_iota(jnp.int32, (n_q, 128), 1)
    far = got2[1, q4]
    far = jnp.where(lane_id % 64 < q4, got2[0, q4], pltpu.roll(far, q4, 1))
    maxes = [mine_ref[2 * q4], sib_ref[2 * q4], far]
    sums = [pltpu.roll(m, 64, 1) for m in maxes]
    top = jnp.maximum(jnp.maximum(maxes[0], maxes[1]), maxes[2])
    factors = [jnp.exp(m - top) for m in maxes]
    inv = 1.0 / (sums[0] * factors[0] + sums[1] * factors[1] + sums[2] * factors[2])
    factors = [f * inv for f in factors]
    for i in range(2 * q4):
        f0, f1, f2 = (jnp.broadcast_to(f[:, i:i + 1], (n_q, 128)) for f in factors)
        att[i] = mine_ref[i] * f0 + sib_ref[i] * f1 + got2[i // q4, i % q4] * f2
    for n in range(n_q):
        lhs[:, n * 128:(n + 1) * 128] = att[:, n, :].astype(jnp.bfloat16)

    y_copy, x_copy, d_copy, e_copy = [], [], [], []
    for t in range(DOTS):
        w_copy(t).wait()
        prod = jnp.dot(lhs[...], w_buf[:, t * wc:(t + 1) * wc], preferred_element_type=jnp.float32)
        if t == 0:
            pl.semaphore_wait(barrier, 3)
        for k in range(per_dot):
            j = t * per_dot + k
            part[j] = prod[:, k * cc:(k + 1) * cc]
            y_copy.append(remote(part.at[j], y_in.at[j], ys_sem.at[j], yr_sem.at[j], yn))
            y_copy[j].start()

    my_rows = pl.ds(pl.multiple_of(x * (2 * q4), 2 * q4), 2 * q4)
    xn_rows = pl.ds(pl.multiple_of((1 - x) * (2 * q4), 2 * q4), 2 * q4)

    def cols(start, j):
        return pl.ds(pl.multiple_of(start + j * cc, 128), cc)

    for j in range(OUT_CHUNKS):
        y_copy[j].wait_recv()
        fin[j] = h_ref[my_rows, cols(own_col, j)].astype(jnp.float32) + (part[j] + y_in[j])
        x_copy.append(remote(fin.at[j], x_in.at[j], xs_sem.at[j], xr_sem.at[j], xn))
        x_copy[j].start()
        d_copy.append(remote(fin.at[j], d_in.at[j], ds_sem.at[j], dr_sem.at[j], sib))
        d_copy[j].start()
        out_ref[my_rows, cols(own_col, j)] = fin[j].astype(jnp.bfloat16)
    for j in range(OUT_CHUNKS):
        x_copy[j].wait_recv()
        e_copy.append(remote(x_in.at[j], d_in2.at[j], es_sem.at[j], er_sem.at[j], sib))
        e_copy[j].start()
        out_ref[xn_rows, cols(own_col, j)] = x_in[j].astype(jnp.bfloat16)
        d_copy[j].wait_recv()
        out_ref[my_rows, cols(oth_col, j)] = d_in[j].astype(jnp.bfloat16)
    for j in range(OUT_CHUNKS):
        e_copy[j].wait_recv()
        out_ref[xn_rows, cols(oth_col, j)] = d_in2[j].astype(jnp.bfloat16)

    for cp in y_copy + x_copy + d_copy + e_copy:
        cp.wait_send()


def solution(mesh):
    cache_spec = P('dp', 'sp', 'tp', None)

    def local_step(hidden, norm_scale, w_qkv, w_out, k_cache, v_cache, positions):
        n_seq, seq_local, kv_local, head = k_cache.shape
        d_model = hidden.shape[1]
        rows = seq_local * kv_local
        n_q = 4 * kv_local
        q4 = n_seq // 4
        vm = pl.BlockSpec(memory_space=pltpu.VMEM)
        hbm = pl.BlockSpec(memory_space=pltpu.HBM)
        dma = pltpu.SemaphoreType.DMA
        f32, bf16 = jnp.float32, jnp.bfloat16
        payload = pltpu.VMEM((q4 + 1, n_q, head), f32)
        payload2 = pltpu.VMEM((2 * q4 + 1, n_q, head), f32)
        k_rows = k_cache.reshape(n_seq, rows, head)
        v_rows = v_cache.reshape(n_seq, rows, head)
        slots = n_seq // PART
        late = pltpu.VMEM((n_seq - EARLY_PARTS * PART, rows, head), bf16)
        w_chunks = len(W_SPLIT)

        def pin(a):
            return pltpu.with_memory_space_constraint(a, pltpu.HBM)

        k_all, v_all, pay, q_own, kn, vn = pl.pallas_call(
            first_kernel,
            out_shape=(pltpu.VMEM((n_seq, rows, head), bf16), pltpu.VMEM((n_seq, rows, head), bf16),
                       payload,
                       pltpu.VMEM((2 * q4, n_q, head), f32), pltpu.VMEM((n_seq, 8, head), f32),
                       pltpu.VMEM((n_seq, 8, head), f32)),
            in_specs=[hbm] * 6,
            out_specs=(vm,) * 6,
            scratch_shapes=[
                pltpu.SMEM((n_seq,), jnp.int32),
                pltpu.VMEM((n_seq, d_model), bf16),
                pltpu.VMEM((d_model // 128, 128), bf16),
                pltpu.VMEM((d_model, 3 * kv_local * head), bf16),
                pltpu.VMEM((n_seq, d_model), bf16),
                pltpu.VMEM((6 * kv_local, n_seq, head), f32),
                pltpu.VMEM((n_seq // 2, n_q, head), f32),
                pltpu.VMEM((n_seq, head), f32),
                pltpu.VMEM((n_q, rows), jnp.int32),
                pltpu.VMEM((2, PART, n_q, rows), f32),
                payload, payload,
                dma((3,)), dma((w_chunks,)), dma((slots,)), dma((slots,)),
                dma((w_chunks + 1,)), dma((w_chunks + 1,)),
            ],
            compiler_params=pltpu.CompilerParams(
                collective_id=1, has_side_effects=True, vmem_limit_bytes=FIRST_VMEM * 1024 * 1024),
            cost_estimate=pl.CostEstimate(flops=2 * 10**10, bytes_accessed=4 * 10**7, transcendentals=0),
            name='first',
        )(*map(pin, (positions, hidden, norm_scale.reshape(d_model // 128, 128), w_qkv, k_rows, v_rows)))

        got = lax.ppermute(pay, 'sp', [(i, i ^ 2) for i in range(4)])

        k_part, v_part, mine, k_late, v_late = pl.pallas_call(
            second_kernel,
            out_shape=(jax.ShapeDtypeStruct((n_seq, rows, head), bf16),
                       jax.ShapeDtypeStruct((n_seq, rows, head), bf16), payload2, late, late),
            in_specs=[hbm, vm, vm, vm, vm, vm],
            out_specs=(hbm, hbm, vm, vm, vm),
            scratch_shapes=[
                pltpu.SMEM((n_seq,), jnp.int32),
                pltpu.VMEM((n_q, rows), jnp.int32),
                pltpu.VMEM((2, PART, n_q, rows), f32),
                dma((1,)), dma((2, n_seq // PART)),
            ],
            compiler_params=pltpu.CompilerParams(vmem_limit_bytes=12 * 1024 * 1024),
            cost_estimate=pl.CostEstimate(flops=2 * 10**10, bytes_accessed=4 * 10**7, transcendentals=0),
            name='second',
        )(positions, q_own, kn, vn, k_all, v_all)

        swap = [(i, i ^ 1) for i in range(4)]
        sib_mine = lax.ppermute(mine, 'sp', swap)
        sib_got = lax.ppermute(got, 'sp', swap)

        k_upd, v_upd = pl.pallas_call(
            third_kernel,
            out_shape=(jax.ShapeDtypeStruct((n_seq, rows, head), bf16),
                       jax.ShapeDtypeStruct((n_seq, rows, head), bf16)),
            in_specs=[vm, vm, hbm, hbm],
            out_specs=(hbm, hbm),
            input_output_aliases={2: 0, 3: 1},
            scratch_shapes=[dma((2, n_seq // PART))],
            compiler_params=pltpu.CompilerParams(vmem_limit_bytes=12 * 1024 * 1024),
            cost_estimate=pl.CostEstimate(flops=2 * 10**10, bytes_accessed=4 * 10**7, transcendentals=0),
            name='third',
        )(k_late, v_late, k_part, v_part)

        half_cols = d_model // 2
        cc = half_cols // OUT_CHUNKS
        chunk = pltpu.VMEM((OUT_CHUNKS, 2 * q4, cc), f32)
        h_out = pl.pallas_call(
            finish_kernel,
            out_shape=jax.ShapeDtypeStruct((n_seq, d_model), bf16),
            in_specs=[vm, hbm, vm, vm, vm, vm],
            out_specs=vm,
            scratch_shapes=[
                pltpu.VMEM((w_out.shape[0], half_cols), bf16),
                pltpu.VMEM((2 * q4, n_q, head), f32),
                pltpu.VMEM((2, q4 + 1, n_q, head), f32),
                pltpu.VMEM((2 * q4, n_q * head), bf16),
                chunk, chunk, chunk, chunk, chunk, chunk,
                dma((DOTS,)),
                dma((OUT_CHUNKS,)), dma((OUT_CHUNKS,)),
                dma((OUT_CHUNKS,)), dma((OUT_CHUNKS,)),
                dma((OUT_CHUNKS,)), dma((OUT_CHUNKS,)),
                dma((OUT_CHUNKS,)), dma((OUT_CHUNKS,)),
            ],
            compiler_params=pltpu.CompilerParams(
                collective_id=0, has_side_effects=True, vmem_limit_bytes=50 * 1024 * 1024),
            name='finish',
        )(hidden, pin(w_out), mine, sib_mine, got, sib_got)
        return h_out, k_upd.reshape(k_cache.shape), v_upd.reshape(v_cache.shape)

    return jax.shard_map(
        local_step,
        mesh=mesh,
        in_specs=(P('dp', None), P(None), P(None, 'tp'), P('tp', None), cache_spec, cache_spec, P('dp')),
        out_specs=(P('dp', None), cache_spec, cache_spec),
        check_vma=False,
    )
```

```python
import math

import jax
import jax.numpy as jnp
from jax import lax
from jax.experimental import pallas as pl
from jax.experimental.pallas import tpu as pltpu
from jax.sharding import PartitionSpec as P

MESH = pl.DeviceIdType.MESH
NEG = -1e30
PV_LAG = 8
W_SPLIT = (4, 4, 4)
PART = 8
EARLY_PARTS = 7
DOTS = 8
OUT_CHUNKS = 8
LN_EPS = 1e-5
FIRST_VMEM = 36


def quarters(n_seq):
    sp = lax.axis_index('sp')
    x, c = sp // 2, sp % 2
    q = n_seq // 4

    def start(xx, cc):
        return pl.multiple_of((xx * 2 + cc) * q, q)
    own = start(x, 0)
    return [start(1 - x, 1 - c), start(1 - x, c), own, pl.multiple_of(own + q, q)]


def insert_row(k_ref, v_ref, at_b, p, kn, vn):
    rows, head = k_ref.shape[1:]
    kv_local = rows // 128
    per = 16 // kv_local
    tile = jnp.clip(p // per, 0, rows // 16 - 1)
    at = pl.ds(pl.multiple_of(tile * 16, 16), 16)
    hit = lax.broadcasted_iota(jnp.int32, (16, head), 0) // kv_local == p - tile * per
    kn, vn = (jnp.concatenate([new[:kv_local]] * per, axis=0) for new in (kn, vn))
    k_ref[at_b, at, :] = jnp.where(hit, kn, k_ref[at_b, at, :].astype(jnp.float32)).astype(jnp.bfloat16)
    v_ref[at_b, at, :] = jnp.where(hit, vn, v_ref[at_b, at, :].astype(jnp.float32)).astype(jnp.bfloat16)


def write_copies(i, starts, q4, k_ref, v_ref, ko_ref, vo_ref, sem, first=0):
    at = i * PART
    src = pl.ds(at - first * PART, PART)
    dst = pl.ds(starts[at // q4] + at % q4, PART)
    return (pltpu.make_async_copy(k_ref.at[src], ko_ref.at[dst], sem.at[0, i]),
            pltpu.make_async_copy(v_ref.at[src], vo_ref.at[dst], sem.at[1, i]))


def insert_part(i, starts, base, pos_ref, k_ref, v_ref, kn_ref, vn_ref):
    q4 = k_ref.shape[0] // 4
    for k in range(i * PART, (i + 1) * PART):
        b = starts[k // q4] + k % q4
        insert_row(k_ref, v_ref, k, pos_ref[b] - base, kn_ref[b], vn_ref[b])


def row_index(n_q, rows):
    kv_local = n_q // 4
    col = lax.broadcasted_iota(jnp.int32, (n_q, rows), 1)
    qg = lax.broadcasted_iota(jnp.int32, (n_q, rows), 0) // 4
    return jnp.where(col % kv_local == qg, col // kv_local, 1 << 20)


def attend_parts(parts, arrive, q_at, p_at, k_ref, v_ref, idx_ref, s_ref, out_at):
    scale = k_ref.shape[2] ** -0.5

    def scores(b, slot, k):
        s_ref[slot, k] = lax.dot_general(
            q_at(b).astype(jnp.bfloat16), k_ref[b], (((1,), (1,)), ((), ())),
            preferred_element_type=jnp.float32)

    arrive(0)
    for k, b in enumerate(parts[0]):
        scores(b, 0, k)
    for i, part in enumerate(parts):
        more = i + 1 < len(parts)
        if more:
            arrive(i + 1)
        held = [None] * len(part)
        for k in range(len(part) + PV_LAG):
            if k < len(part):
                if more:
                    scores(parts[i + 1][k], (i + 1) % 2, k)
                s = jnp.where(idx_ref[...] <= p_at(part[k]), s_ref[i % 2, k] * scale, NEG)
                m = jnp.max(s, axis=1, keepdims=True)
                e = jnp.exp(s - m)
                held[k] = (e.astype(jnp.bfloat16), m, jnp.sum(e, axis=1, keepdims=True))
            if k >= PV_LAG:
                b = part[k - PV_LAG]
                e, m, l = held[k - PV_LAG]
                out_at(b, jnp.dot(e, v_ref[b], preferred_element_type=jnp.float32), m, l)


def put_stats(tile, lane_id, k, m, l):
    return jnp.where(lane_id == k, m, jnp.where(lane_id == 64 + k, l, tile))


def first_kernel(pos_hbm, h_hbm, scale_hbm, w_ref, kc_ref, vc_ref,
                 k_ref, v_ref, pay_ref, q_own, kn_ref, vn_ref,
                 pos_ref, h_ref, scale_ref, w_buf, u_ref, qkv_ref, q_ref,
                 ang_ref, idx_ref, s_ref, out_pay, sib_pay,
                 in_sem, w_sem, k_sem, v_sem, send_sem, recv_sem):
    n_seq, d_model = h_ref.shape
    rows = k_ref.shape[1]
    head = k_ref.shape[2]
    w_chunks = len(W_SPLIT)
    half_heads = w_buf.shape[1] // head
    first_head = [sum(W_SPLIT[:t]) for t in range(w_chunks + 1)]
    n_q = q_ref.shape[1]
    kv_local = n_q // 4
    sp = lax.axis_index('sp')
    core = sp % 2
    sib = {'sp': sp + 1 - 2 * core}
    base = sp * (rows // kv_local)
    starts = quarters(n_seq)
    q4 = n_seq // 4
    per_slot = q4 // PART

    small = [pltpu.make_async_copy(h_hbm, h_ref, in_sem.at[0]),
             pltpu.make_async_copy(scale_hbm, scale_ref, in_sem.at[1]),
             pltpu.make_async_copy(pos_hbm, pos_ref, in_sem.at[2])]
    for cp in small:
        cp.start()

    def w_copy(t):
        at, width = first_head[t] * head, W_SPLIT[t] * head
        src = pl.ds(pl.multiple_of(core * half_heads * head + at, 128), width)
        return pltpu.make_async_copy(w_ref.at[:, src], w_buf.at[:, pl.ds(at, width)], w_sem.at[t])

    def c_copies(i):
        src = pl.ds(starts[i // per_slot] + (i % per_slot) * PART, PART)
        dst = pl.ds(i * PART, PART)
        return (pltpu.make_async_copy(kc_ref.at[src], k_ref.at[dst], k_sem.at[i]),
                pltpu.make_async_copy(vc_ref.at[src], v_ref.at[dst], v_sem.at[i]))

    for t in range(w_chunks):
        w_copy(t).start()

    barrier = pltpu.get_barrier_semaphore()
    pl.semaphore_signal(barrier, inc=1, device_id=sib, device_id_type=MESH)

    idx_ref[...] = row_index(n_q, rows)

    lane = lax.broadcasted_iota(jnp.int32, (1, head), 1)
    half = head // 2
    inv_freq = jnp.exp((lane % half).astype(jnp.float32) * (-2.0 * math.log(500000.0) / head))
    small[2].wait()

    def fill(b, _):
        ang_ref[pl.ds(b, 1), :] = jnp.full((1, head), pos_ref[b].astype(jnp.float32)) * inv_freq
        return 0
    lax.fori_loop(0, n_seq, fill, 0)
    cos = jnp.cos(ang_ref[...])
    sin = jnp.sin(ang_ref[...]) * jnp.where(lane < half, -1.0, 1.0)

    def rope(x):
        return (x * cos + pltpu.roll(x, half, 1) * sin).astype(jnp.bfloat16).astype(jnp.float32)

    small[0].wait()
    small[1].wait()
    blocks = d_model // 128
    total = jnp.zeros((n_seq, 128), jnp.float32)
    for i in range(blocks):
        total += h_ref[:, i * 128:(i + 1) * 128].astype(jnp.float32)
    mean = jnp.sum(total, axis=1, keepdims=True) * (1.0 / d_model)
    total = jnp.zeros((n_seq, 128), jnp.float32)
    for i in range(blocks):
        cen = h_ref[:, i * 128:(i + 1) * 128].astype(jnp.float32) - mean
        total += cen * cen
    var = jnp.sum(total, axis=1, keepdims=True) * (1.0 / d_model)
    rstd = lax.rsqrt(var + LN_EPS)
    for i in range(blocks):
        cen = h_ref[:, i * 128:(i + 1) * 128].astype(jnp.float32) - mean
        u_ref[:, i * 128:(i + 1) * 128] = (
            cen * rstd * scale_ref[i:i + 1, :].astype(jnp.float32)).astype(jnp.bfloat16)
    pl.semaphore_wait(barrier, 1)

    sends = []
    for t in range(w_chunks):
        w_copy(t).wait()
        if t == 0:
            for i in range(4 * per_slot):
                for c in c_copies(i):
                    c.start(priority=1)
        acc = jnp.dot(u_ref[...], w_buf[:, first_head[t] * head:first_head[t + 1] * head],
                      preferred_element_type=jnp.float32)
        qkv = jnp.clip(acc.astype(jnp.bfloat16).astype(jnp.float32), -8.0, 8.0)
        at = core * half_heads + first_head[t]
        for j in range(W_SPLIT[t]):
            val = qkv[:, j * head:(j + 1) * head]
            qkv_ref[at + j] = rope(val) if (first_head[t] + j) % 6 < 5 else val
        block = qkv_ref.at[pl.ds(at, W_SPLIT[t])]
        sends.append(pltpu.make_async_remote_copy(
            src_ref=block, dst_ref=block, send_sem=send_sem.at[t], recv_sem=recv_sem.at[t],
            device_id=sib, device_id_type=MESH))
        sends[t].start()
    half_seq = n_seq // 2
    far_half = pl.ds(pl.multiple_of(half_seq - starts[2], half_seq), half_seq)
    own_half = pl.ds(starts[2], half_seq)
    for t in range(w_chunks):
        sends[t].wait_recv()
        for j in range(first_head[t], first_head[t + 1]):
            for at in (j, half_heads + j):
                g, kind = divmod(at, 6)
                if kind < 4:
                    q_ref[:, g * 4 + kind, :] = qkv_ref[at, far_half]

    lane_id = lax.broadcasted_iota(jnp.int32, (n_q, 128), 1)
    pays = [out_pay, pay_ref]
    stats = [jnp.zeros((n_q, 128), jnp.float32) for _ in pays]
    pay_copy = pltpu.make_async_remote_copy(
        src_ref=out_pay, dst_ref=sib_pay, send_sem=send_sem.at[w_chunks], recv_sem=recv_sem.at[w_chunks],
        device_id=sib, device_id_type=MESH)

    def seq(b):
        return starts[b // q4] + b % q4

    def arrive(i):
        for c in c_copies(i):
            c.wait()

    def out_at(b, o, m, l):
        if b < 6 * kv_local:
            g, kind = divmod(b, 6)
            if kind < 4:
                q_own[:, g * 4 + kind, :] = qkv_ref[b, own_half]
            else:
                (kn_ref, vn_ref)[kind - 4][:, g, :] = qkv_ref[b]
        slot = b // q4
        pays[slot][b % q4] = o
        stats[slot] = put_stats(stats[slot], lane_id, b % q4, m, l)
        if b == q4 - 1:
            out_pay[q4] = stats[0]
            pay_copy.start()

    parts = [list(range(i * PART, (i + 1) * PART)) for i in range(2 * per_slot)]
    attend_parts(parts, arrive, lambda b: q_ref[seq(b) - half_seq + starts[2]], lambda b: pos_ref[seq(b)] - base - 1,
                 k_ref, v_ref, idx_ref, s_ref, out_at)

    pay_copy.wait_recv()
    other = sib_pay[q4]
    top = jnp.maximum(stats[1], other)
    f0, f1 = jnp.exp(stats[1] - top), jnp.exp(other - top)
    total = pltpu.roll(stats[1], 64, 1) * f0 + pltpu.roll(other, 64, 1) * f1
    pay_ref[q4] = jnp.where(lane_id < 64, top, pltpu.roll(total, 64, 1))
    for i in range(q4):
        pay_ref[i] = (pay_ref[i] * jnp.broadcast_to(f0[:, i:i + 1], (n_q, 128))
                      + sib_pay[i] * jnp.broadcast_to(f1[:, i:i + 1], (n_q, 128)))
    for i in range(2 * per_slot, 4 * per_slot):
        arrive(i)
    for cp in sends + [pay_copy]:
        cp.wait_send()


def second_kernel(pos_hbm, q_ref, kn_ref, vn_ref, k_ref, v_ref,
                  ko_ref, vo_ref, pay_ref, k_late, v_late,
                  pos_ref, idx_ref, s_ref,
                  in_sem, o_sem):
    n_seq, rows, head = k_ref.shape
    half_seq, n_q = q_ref.shape[:2]
    kv_local = n_q // 4
    sp = lax.axis_index('sp')
    core = sp % 2
    base = sp * (rows // kv_local)
    starts = quarters(n_seq)
    q4 = n_seq // 4

    pos_copy = pltpu.make_async_copy(pos_hbm, pos_ref, in_sem.at[0])
    pos_copy.start()
    idx_ref[...] = row_index(n_q, rows)
    pos_copy.wait()

    for i in range(EARLY_PARTS):
        insert_part(i, starts, base, pos_ref, k_ref, v_ref, kn_ref, vn_ref)
        for c in write_copies(i, starts, q4, k_ref, v_ref, ko_ref, vo_ref, o_sem):
            c.start()

    late = EARLY_PARTS * PART

    def late_row(k):
        k_late[k - late] = k_ref[k]
        v_late[k - late] = v_ref[k]
        b = starts[k // q4] + k % q4
        insert_row(k_late, v_late, k - late, pos_ref[b] - base, kn_ref[b], vn_ref[b])

    lane_id = lax.broadcasted_iota(jnp.int32, (n_q, 128), 1)
    stats = [jnp.zeros((n_q, 128), jnp.float32)]

    def per_head(tile):
        return jnp.concatenate([jnp.broadcast_to(tile[g:g + 1], (4, head)) for g in range(kv_local)], axis=0)

    def out_at(b, o, m, l):
        k = b - half_seq
        at = starts[2] + k
        s = jnp.sum(q_ref[k] * per_head(kn_ref[at]), axis=1, keepdims=True) * head ** -0.5
        s = jnp.where(core == k // q4, s, NEG)
        top = jnp.maximum(m, s)
        old = jnp.exp(m - top)
        new = jnp.where(core == k // q4, jnp.exp(s - top), 0.0)
        pay_ref[k] = o * old + new.astype(jnp.bfloat16).astype(jnp.float32) * per_head(vn_ref[at])
        stats[0] = put_stats(stats[0], lane_id, k, top, l * old + new)
        if b >= late:
            late_row(b)

    parts = [list(range(half_seq + i, half_seq + i + PART)) for i in range(0, half_seq, PART)]
    attend_parts(parts, lambda i: None, lambda b: q_ref[b - half_seq],
                 lambda b: pos_ref[starts[2] + b - half_seq] - base - 1,
                 k_ref, v_ref, idx_ref, s_ref, out_at)
    pay_ref[half_seq] = stats[0]
    for i in range(EARLY_PARTS):
        for c in write_copies(i, starts, q4, k_ref, v_ref, ko_ref, vo_ref, o_sem):
            c.wait()


def third_kernel(k_late, v_late, k_in, v_in, ko_ref, vo_ref, o_sem):
    n_seq = ko_ref.shape[0]
    starts = quarters(n_seq)
    parts = range(EARLY_PARTS, n_seq // PART)
    for i in parts:
        for c in write_copies(i, starts, n_seq // 4, k_late, v_late, ko_ref, vo_ref, o_sem, EARLY_PARTS):
            c.start()
    for i in parts:
        for c in write_copies(i, starts, n_seq // 4, k_late, v_late, ko_ref, vo_ref, o_sem, EARLY_PARTS):
            c.wait()


def finish_kernel(h_ref, w_ref, mine_ref, sib_ref, got_ref, sib_got_ref, out_ref,
                  w_buf, att, got2, lhs, part, y_in, fin, x_in, d_in, d_in2,
                  w_sem, ys_sem, yr_sem, xs_sem, xr_sem, ds_sem, dr_sem, es_sem, er_sem):
    n_q = mine_ref.shape[1]
    sp = lax.axis_index('sp')
    tp = lax.axis_index('tp')
    x, c = sp // 2, sp % 2
    sib = {'sp': x * 2 + (1 - c)}
    xn = {'sp': (1 - x) * 2 + c}
    yn = {'tp': 1 - tp}

    half_cols = w_buf.shape[1]
    cc = half_cols // OUT_CHUNKS
    q4 = got_ref.shape[0] - 1
    own_col = c * half_cols
    oth_col = (1 - c) * half_cols

    wc = half_cols // DOTS
    per_dot = OUT_CHUNKS // DOTS

    def w_copy(j):
        return pltpu.make_async_copy(
            w_ref.at[:, pl.ds(pl.multiple_of(own_col + j * wc, 128), wc)],
            w_buf.at[:, pl.ds(j * wc, wc)], w_sem.at[j])

    for j in range(DOTS):
        w_copy(j).start()

    barrier = pltpu.get_barrier_semaphore()
    for dev in (sib, xn, yn):
        pl.semaphore_signal(barrier, inc=1, device_id=dev, device_id_type=MESH)

    def remote(src, dst, ssem, rsem, dev):
        return pltpu.make_async_remote_copy(src_ref=src, dst_ref=dst, send_sem=ssem, recv_sem=rsem,
                                            device_id=dev, device_id_type=MESH)

    got2[c] = got_ref[...]
    got2[1 - c] = sib_got_ref[...]

    lane_id = lax.broadcasted_iota(jnp.int32, (n_q, 128), 1)
    far = got2[1, q4]
    far = jnp.where(lane_id % 64 < q4, got2[0, q4], pltpu.roll(far, q4, 1))
    maxes = [mine_ref[2 * q4], sib_ref[2 * q4], far]
    sums = [pltpu.roll(m, 64, 1) for m in maxes]
    top = jnp.maximum(jnp.maximum(maxes[0], maxes[1]), maxes[2])
    factors = [jnp.exp(m - top) for m in maxes]
    inv = 1.0 / (sums[0] * factors[0] + sums[1] * factors[1] + sums[2] * factors[2])
    factors = [f * inv for f in factors]
    for i in range(2 * q4):
        f0, f1, f2 = (jnp.broadcast_to(f[:, i:i + 1], (n_q, 128)) for f in factors)
        att[i] = mine_ref[i] * f0 + sib_ref[i] * f1 + got2[i // q4, i % q4] * f2
    for n in range(n_q):
        lhs[:, n * 128:(n + 1) * 128] = att[:, n, :].astype(jnp.bfloat16)

    y_copy, x_copy, d_copy, e_copy = [], [], [], []
    for t in range(DOTS):
        w_copy(t).wait()
        prod = jnp.dot(lhs[...], w_buf[:, t * wc:(t + 1) * wc], preferred_element_type=jnp.float32)
        if t == 0:
            pl.semaphore_wait(barrier, 3)
        for k in range(per_dot):
            j = t * per_dot + k
            part[j] = prod[:, k * cc:(k + 1) * cc]
            y_copy.append(remote(part.at[j], y_in.at[j], ys_sem.at[j], yr_sem.at[j], yn))
            y_copy[j].start()

    my_rows = pl.ds(pl.multiple_of(x * (2 * q4), 2 * q4), 2 * q4)
    xn_rows = pl.ds(pl.multiple_of((1 - x) * (2 * q4), 2 * q4), 2 * q4)

    def cols(start, j):
        return pl.ds(pl.multiple_of(start + j * cc, 128), cc)

    for j in range(OUT_CHUNKS):
        y_copy[j].wait_recv()
        fin[j] = h_ref[my_rows, cols(own_col, j)].astype(jnp.float32) + (part[j] + y_in[j])
        x_copy.append(remote(fin.at[j], x_in.at[j], xs_sem.at[j], xr_sem.at[j], xn))
        x_copy[j].start()
        d_copy.append(remote(fin.at[j], d_in.at[j], ds_sem.at[j], dr_sem.at[j], sib))
        d_copy[j].start()
        out_ref[my_rows, cols(own_col, j)] = fin[j].astype(jnp.bfloat16)
    for j in range(OUT_CHUNKS):
        x_copy[j].wait_recv()
        e_copy.append(remote(x_in.at[j], d_in2.at[j], es_sem.at[j], er_sem.at[j], sib))
        e_copy[j].start()
        out_ref[xn_rows, cols(own_col, j)] = x_in[j].astype(jnp.bfloat16)
        d_copy[j].wait_recv()
        out_ref[my_rows, cols(oth_col, j)] = d_in[j].astype(jnp.bfloat16)
    for j in range(OUT_CHUNKS):
        e_copy[j].wait_recv()
        out_ref[xn_rows, cols(oth_col, j)] = d_in2[j].astype(jnp.bfloat16)

    for cp in y_copy + x_copy + d_copy + e_copy:
        cp.wait_send()


def solution(mesh):
    cache_spec = P('dp', 'sp', 'tp', None)

    def local_step(hidden, norm_scale, w_qkv, w_out, k_cache, v_cache, positions):
        n_seq, seq_local, kv_local, head = k_cache.shape
        d_model = hidden.shape[1]
        rows = seq_local * kv_local
        n_q = 4 * kv_local
        q4 = n_seq // 4
        vm = pl.BlockSpec(memory_space=pltpu.VMEM)
        hbm = pl.BlockSpec(memory_space=pltpu.HBM)
        dma = pltpu.SemaphoreType.DMA
        f32, bf16 = jnp.float32, jnp.bfloat16
        payload = pltpu.VMEM((q4 + 1, n_q, head), f32)
        payload2 = pltpu.VMEM((2 * q4 + 1, n_q, head), f32)
        k_rows = k_cache.reshape(n_seq, rows, head)
        v_rows = v_cache.reshape(n_seq, rows, head)
        slots = n_seq // PART
        late = pltpu.VMEM((n_seq - EARLY_PARTS * PART, rows, head), bf16)
        w_chunks = len(W_SPLIT)

        def pin(a):
            return pltpu.with_memory_space_constraint(a, pltpu.HBM)

        k_all, v_all, pay, q_own, kn, vn = pl.pallas_call(
            first_kernel,
            out_shape=(pltpu.VMEM((n_seq, rows, head), bf16), pltpu.VMEM((n_seq, rows, head), bf16),
                       payload,
                       pltpu.VMEM((2 * q4, n_q, head), f32), pltpu.VMEM((n_seq, 8, head), f32),
                       pltpu.VMEM((n_seq, 8, head), f32)),
            in_specs=[hbm] * 6,
            out_specs=(vm,) * 6,
            scratch_shapes=[
                pltpu.SMEM((n_seq,), jnp.int32),
                pltpu.VMEM((n_seq, d_model), bf16),
                pltpu.VMEM((d_model // 128, 128), bf16),
                pltpu.VMEM((d_model, 3 * kv_local * head), bf16),
                pltpu.VMEM((n_seq, d_model), bf16),
                pltpu.VMEM((6 * kv_local, n_seq, head), f32),
                pltpu.VMEM((n_seq // 2, n_q, head), f32),
                pltpu.VMEM((n_seq, head), f32),
                pltpu.VMEM((n_q, rows), jnp.int32),
                pltpu.VMEM((2, PART, n_q, rows), f32),
                payload, payload,
                dma((3,)), dma((w_chunks,)), dma((slots,)), dma((slots,)),
                dma((w_chunks + 1,)), dma((w_chunks + 1,)),
            ],
            compiler_params=pltpu.CompilerParams(
                collective_id=1, has_side_effects=True, vmem_limit_bytes=FIRST_VMEM * 1024 * 1024),
            cost_estimate=pl.CostEstimate(flops=2 * 10**10, bytes_accessed=4 * 10**7, transcendentals=0),
            name='first',
        )(*map(pin, (positions, hidden, norm_scale.reshape(d_model // 128, 128), w_qkv, k_rows, v_rows)))

        got = lax.ppermute(pay, 'sp', [(i, i ^ 2) for i in range(4)])

        k_part, v_part, mine, k_late, v_late = pl.pallas_call(
            second_kernel,
            out_shape=(jax.ShapeDtypeStruct((n_seq, rows, head), bf16),
                       jax.ShapeDtypeStruct((n_seq, rows, head), bf16), payload2, late, late),
            in_specs=[hbm, vm, vm, vm, vm, vm],
            out_specs=(hbm, hbm, vm, vm, vm),
            scratch_shapes=[
                pltpu.SMEM((n_seq,), jnp.int32),
                pltpu.VMEM((n_q, rows), jnp.int32),
                pltpu.VMEM((2, PART, n_q, rows), f32),
                dma((1,)), dma((2, n_seq // PART)),
            ],
            compiler_params=pltpu.CompilerParams(vmem_limit_bytes=12 * 1024 * 1024),
            cost_estimate=pl.CostEstimate(flops=2 * 10**10, bytes_accessed=4 * 10**7, transcendentals=0),
            name='second',
        )(positions, q_own, kn, vn, k_all, v_all)

        swap = [(i, i ^ 1) for i in range(4)]
        sib_mine = lax.ppermute(mine, 'sp', swap)
        sib_got = lax.ppermute(got, 'sp', swap)

        k_upd, v_upd = pl.pallas_call(
            third_kernel,
            out_shape=(jax.ShapeDtypeStruct((n_seq, rows, head), bf16),
                       jax.ShapeDtypeStruct((n_seq, rows, head), bf16)),
            in_specs=[vm, vm, hbm, hbm],
            out_specs=(hbm, hbm),
            input_output_aliases={2: 0, 3: 1},
            scratch_shapes=[dma((2, n_seq // PART))],
            compiler_params=pltpu.CompilerParams(vmem_limit_bytes=12 * 1024 * 1024),
            cost_estimate=pl.CostEstimate(flops=2 * 10**10, bytes_accessed=4 * 10**7, transcendentals=0),
            name='third',
        )(k_late, v_late, k_part, v_part)

        half_cols = d_model // 2
        cc = half_cols // OUT_CHUNKS
        chunk = pltpu.VMEM((OUT_CHUNKS, 2 * q4, cc), f32)
        h_out = pl.pallas_call(
            finish_kernel,
            out_shape=jax.ShapeDtypeStruct((n_seq, d_model), bf16),
            in_specs=[vm, hbm, vm, vm, vm, vm],
            out_specs=vm,
            scratch_shapes=[
                pltpu.VMEM((w_out.shape[0], half_cols), bf16),
                pltpu.VMEM((2 * q4, n_q, head), f32),
                pltpu.VMEM((2, q4 + 1, n_q, head), f32),
                pltpu.VMEM((2 * q4, n_q * head), bf16),
                chunk, chunk, chunk, chunk, chunk, chunk,
                dma((DOTS,)),
                dma((OUT_CHUNKS,)), dma((OUT_CHUNKS,)),
                dma((OUT_CHUNKS,)), dma((OUT_CHUNKS,)),
                dma((OUT_CHUNKS,)), dma((OUT_CHUNKS,)),
                dma((OUT_CHUNKS,)), dma((OUT_CHUNKS,)),
            ],
            compiler_params=pltpu.CompilerParams(
                collective_id=0, has_side_effects=True, vmem_limit_bytes=50 * 1024 * 1024),
            name='finish',
        )(hidden, pin(w_out), mine, sib_mine, got, sib_got)
        return h_out, k_upd.reshape(k_cache.shape), v_upd.reshape(v_cache.shape)

    return jax.shard_map(
        local_step,
        mesh=mesh,
        in_specs=(P('dp', None), P(None), P(None, 'tp'), P('tp', None), cache_spec, cache_spec, P('dp')),
        out_specs=(P('dp', None), cache_spec, cache_spec),
        check_vma=False,
    )
```

```python
import math

import jax
import jax.numpy as jnp
from jax import lax
from jax.experimental import pallas as pl
from jax.experimental.pallas import tpu as pltpu
from jax.sharding import PartitionSpec as P

MESH = pl.DeviceIdType.MESH
NEG = -1e30
PV_LAG = 6
W_SPLIT = (4, 4, 4)
PART = 8
EARLY_PARTS = 7
DOTS = 8
OUT_CHUNKS = 8
LN_EPS = 1e-5
FIRST_VMEM = 36


def quarters(n_seq):
    sp = lax.axis_index('sp')
    x, c = sp // 2, sp % 2
    q = n_seq // 4

    def start(xx, cc):
        return pl.multiple_of((xx * 2 + cc) * q, q)
    own = start(x, 0)
    return [start(1 - x, 1 - c), start(1 - x, c), own, pl.multiple_of(own + q, q)]


def insert_row(k_ref, v_ref, at_b, p, kn, vn):
    rows, head = k_ref.shape[1:]
    kv_local = rows // 128
    per = 16 // kv_local
    tile = jnp.clip(p // per, 0, rows // 16 - 1)
    at = pl.ds(pl.multiple_of(tile * 16, 16), 16)
    hit = lax.broadcasted_iota(jnp.int32, (16, head), 0) // kv_local == p - tile * per
    kn, vn = (jnp.concatenate([new[:kv_local]] * per, axis=0) for new in (kn, vn))
    k_ref[at_b, at, :] = jnp.where(hit, kn, k_ref[at_b, at, :].astype(jnp.float32)).astype(jnp.bfloat16)
    v_ref[at_b, at, :] = jnp.where(hit, vn, v_ref[at_b, at, :].astype(jnp.float32)).astype(jnp.bfloat16)


def write_copies(i, starts, q4, k_ref, v_ref, ko_ref, vo_ref, sem, first=0):
    at = i * PART
    src = pl.ds(at - first * PART, PART)
    dst = pl.ds(starts[at // q4] + at % q4, PART)
    return (pltpu.make_async_copy(k_ref.at[src], ko_ref.at[dst], sem.at[0, i]),
            pltpu.make_async_copy(v_ref.at[src], vo_ref.at[dst], sem.at[1, i]))


def insert_part(i, starts, base, pos_ref, k_ref, v_ref, kn_ref, vn_ref):
    q4 = k_ref.shape[0] // 4
    for k in range(i * PART, (i + 1) * PART):
        b = starts[k // q4] + k % q4
        insert_row(k_ref, v_ref, k, pos_ref[b] - base, kn_ref[b], vn_ref[b])


def row_index(n_q, rows):
    kv_local = n_q // 4
    col = lax.broadcasted_iota(jnp.int32, (n_q, rows), 1)
    qg = lax.broadcasted_iota(jnp.int32, (n_q, rows), 0) // 4
    return jnp.where(col % kv_local == qg, col // kv_local, 1 << 20)


def attend_parts(parts, arrive, q_at, p_at, k_ref, v_ref, idx_ref, s_ref, out_at):
    scale = k_ref.shape[2] ** -0.5

    def scores(b, slot, k):
        s_ref[slot, k] = lax.dot_general(
            q_at(b).astype(jnp.bfloat16), k_ref[b], (((1,), (1,)), ((), ())),
            preferred_element_type=jnp.float32)

    arrive(0)
    for k, b in enumerate(parts[0]):
        scores(b, 0, k)
    for i, part in enumerate(parts):
        more = i + 1 < len(parts)
        if more:
            arrive(i + 1)
        held = [None] * len(part)
        for k in range(len(part) + PV_LAG):
            if k < len(part):
                if more:
                    scores(parts[i + 1][k], (i + 1) % 2, k)
                s = jnp.where(idx_ref[...] <= p_at(part[k]), s_ref[i % 2, k] * scale, NEG)
                m = jnp.max(s, axis=1, keepdims=True)
                e = jnp.exp(s - m)
                held[k] = (e.astype(jnp.bfloat16), m, jnp.sum(e, axis=1, keepdims=True))
            if k >= PV_LAG:
                b = part[k - PV_LAG]
                e, m, l = held[k - PV_LAG]
                out_at(b, jnp.dot(e, v_ref[b], preferred_element_type=jnp.float32), m, l)


def put_stats(tile, lane_id, k, m, l):
    return jnp.where(lane_id == k, m, jnp.where(lane_id == 64 + k, l, tile))


def first_kernel(pos_hbm, h_hbm, scale_hbm, w_ref, kc_ref, vc_ref,
                 k_ref, v_ref, pay_ref, q_own, kn_ref, vn_ref,
                 pos_ref, h_ref, scale_ref, w_buf, u_ref, qkv_ref, q_ref,
                 ang_ref, idx_ref, s_ref, out_pay, sib_pay,
                 in_sem, w_sem, k_sem, v_sem, send_sem, recv_sem):
    n_seq, d_model = h_ref.shape
    rows = k_ref.shape[1]
    head = k_ref.shape[2]
    w_chunks = len(W_SPLIT)
    half_heads = w_buf.shape[1] // head
    first_head = [sum(W_SPLIT[:t]) for t in range(w_chunks + 1)]
    n_q = q_ref.shape[1]
    kv_local = n_q // 4
    sp = lax.axis_index('sp')
    core = sp % 2
    sib = {'sp': sp + 1 - 2 * core}
    base = sp * (rows // kv_local)
    starts = quarters(n_seq)
    q4 = n_seq // 4
    per_slot = q4 // PART

    small = [pltpu.make_async_copy(h_hbm, h_ref, in_sem.at[0]),
             pltpu.make_async_copy(scale_hbm, scale_ref, in_sem.at[1]),
             pltpu.make_async_copy(pos_hbm, pos_ref, in_sem.at[2])]
    for cp in small:
        cp.start()

    def w_copy(t):
        at, width = first_head[t] * head, W_SPLIT[t] * head
        src = pl.ds(pl.multiple_of(core * half_heads * head + at, 128), width)
        return pltpu.make_async_copy(w_ref.at[:, src], w_buf.at[:, pl.ds(at, width)], w_sem.at[t])

    def c_copies(i):
        src = pl.ds(starts[i // per_slot] + (i % per_slot) * PART, PART)
        dst = pl.ds(i * PART, PART)
        return (pltpu.make_async_copy(kc_ref.at[src], k_ref.at[dst], k_sem.at[i]),
                pltpu.make_async_copy(vc_ref.at[src], v_ref.at[dst], v_sem.at[i]))

    for t in range(w_chunks):
        w_copy(t).start()

    barrier = pltpu.get_barrier_semaphore()
    pl.semaphore_signal(barrier, inc=1, device_id=sib, device_id_type=MESH)

    idx_ref[...] = row_index(n_q, rows)

    lane = lax.broadcasted_iota(jnp.int32, (1, head), 1)
    half = head // 2
    inv_freq = jnp.exp((lane % half).astype(jnp.float32) * (-2.0 * math.log(500000.0) / head))
    small[2].wait()

    def fill(b, _):
        ang_ref[pl.ds(b, 1), :] = jnp.full((1, head), pos_ref[b].astype(jnp.float32)) * inv_freq
        return 0
    lax.fori_loop(0, n_seq, fill, 0)
    cos = jnp.cos(ang_ref[...])
    sin = jnp.sin(ang_ref[...]) * jnp.where(lane < half, -1.0, 1.0)

    def rope(x):
        return (x * cos + pltpu.roll(x, half, 1) * sin).astype(jnp.bfloat16).astype(jnp.float32)

    small[0].wait()
    small[1].wait()
    blocks = d_model // 128
    total = jnp.zeros((n_seq, 128), jnp.float32)
    for i in range(blocks):
        total += h_ref[:, i * 128:(i + 1) * 128].astype(jnp.float32)
    mean = jnp.sum(total, axis=1, keepdims=True) * (1.0 / d_model)
    total = jnp.zeros((n_seq, 128), jnp.float32)
    for i in range(blocks):
        cen = h_ref[:, i * 128:(i + 1) * 128].astype(jnp.float32) - mean
        total += cen * cen
    var = jnp.sum(total, axis=1, keepdims=True) * (1.0 / d_model)
    rstd = lax.rsqrt(var + LN_EPS)
    for i in range(blocks):
        cen = h_ref[:, i * 128:(i + 1) * 128].astype(jnp.float32) - mean
        u_ref[:, i * 128:(i + 1) * 128] = (
            cen * rstd * scale_ref[i:i + 1, :].astype(jnp.float32)).astype(jnp.bfloat16)
    pl.semaphore_wait(barrier, 1)

    sends = []
    for t in range(w_chunks):
        w_copy(t).wait()
        if t == 0:
            for i in range(4 * per_slot):
                for c in c_copies(i):
                    c.start(priority=1)
        acc = jnp.dot(u_ref[...], w_buf[:, first_head[t] * head:first_head[t + 1] * head],
                      preferred_element_type=jnp.float32)
        qkv = jnp.clip(acc.astype(jnp.bfloat16).astype(jnp.float32), -8.0, 8.0)
        at = core * half_heads + first_head[t]
        for j in range(W_SPLIT[t]):
            val = qkv[:, j * head:(j + 1) * head]
            qkv_ref[at + j] = rope(val) if (first_head[t] + j) % 6 < 5 else val
        block = qkv_ref.at[pl.ds(at, W_SPLIT[t])]
        sends.append(pltpu.make_async_remote_copy(
            src_ref=block, dst_ref=block, send_sem=send_sem.at[t], recv_sem=recv_sem.at[t],
            device_id=sib, device_id_type=MESH))
        sends[t].start()
    half_seq = n_seq // 2
    far_half = pl.ds(pl.multiple_of(half_seq - starts[2], half_seq), half_seq)
    own_half = pl.ds(starts[2], half_seq)
    for t in range(w_chunks):
        sends[t].wait_recv()
        for j in range(first_head[t], first_head[t + 1]):
            for at in (j, half_heads + j):
                g, kind = divmod(at, 6)
                if kind < 4:
                    q_ref[:, g * 4 + kind, :] = qkv_ref[at, far_half]

    lane_id = lax.broadcasted_iota(jnp.int32, (n_q, 128), 1)
    pays = [out_pay, pay_ref]
    stats = [jnp.zeros((n_q, 128), jnp.float32) for _ in pays]
    pay_copy = pltpu.make_async_remote_copy(
        src_ref=out_pay, dst_ref=sib_pay, send_sem=send_sem.at[w_chunks], recv_sem=recv_sem.at[w_chunks],
        device_id=sib, device_id_type=MESH)

    def seq(b):
        return starts[b // q4] + b % q4

    def arrive(i):
        for c in c_copies(i):
            c.wait()

    def out_at(b, o, m, l):
        if b < 6 * kv_local:
            g, kind = divmod(b, 6)
            if kind < 4:
                q_own[:, g * 4 + kind, :] = qkv_ref[b, own_half]
            else:
                (kn_ref, vn_ref)[kind - 4][:, g, :] = qkv_ref[b]
        slot = b // q4
        pays[slot][b % q4] = o
        stats[slot] = put_stats(stats[slot], lane_id, b % q4, m, l)
        if b == q4 - 1:
            out_pay[q4] = stats[0]
            pay_copy.start()

    parts = [list(range(i * PART, (i + 1) * PART)) for i in range(2 * per_slot)]
    attend_parts(parts, arrive, lambda b: q_ref[seq(b) - half_seq + starts[2]], lambda b: pos_ref[seq(b)] - base - 1,
                 k_ref, v_ref, idx_ref, s_ref, out_at)

    pay_copy.wait_recv()
    other = sib_pay[q4]
    top = jnp.maximum(stats[1], other)
    f0, f1 = jnp.exp(stats[1] - top), jnp.exp(other - top)
    total = pltpu.roll(stats[1], 64, 1) * f0 + pltpu.roll(other, 64, 1) * f1
    pay_ref[q4] = jnp.where(lane_id < 64, top, pltpu.roll(total, 64, 1))
    for i in range(q4):
        pay_ref[i] = (pay_ref[i] * jnp.broadcast_to(f0[:, i:i + 1], (n_q, 128))
                      + sib_pay[i] * jnp.broadcast_to(f1[:, i:i + 1], (n_q, 128)))
    for i in range(2 * per_slot, 4 * per_slot):
        arrive(i)
    for cp in sends + [pay_copy]:
        cp.wait_send()


def second_kernel(pos_hbm, q_ref, kn_ref, vn_ref, k_ref, v_ref,
                  ko_ref, vo_ref, pay_ref, k_late, v_late,
                  pos_ref, idx_ref, s_ref,
                  in_sem, o_sem):
    n_seq, rows, head = k_ref.shape
    half_seq, n_q = q_ref.shape[:2]
    kv_local = n_q // 4
    sp = lax.axis_index('sp')
    core = sp % 2
    base = sp * (rows // kv_local)
    starts = quarters(n_seq)
    q4 = n_seq // 4

    pos_copy = pltpu.make_async_copy(pos_hbm, pos_ref, in_sem.at[0])
    pos_copy.start()
    idx_ref[...] = row_index(n_q, rows)
    pos_copy.wait()

    for i in range(EARLY_PARTS):
        insert_part(i, starts, base, pos_ref, k_ref, v_ref, kn_ref, vn_ref)
        for c in write_copies(i, starts, q4, k_ref, v_ref, ko_ref, vo_ref, o_sem):
            c.start()

    late = EARLY_PARTS * PART

    def late_row(k):
        k_late[k - late] = k_ref[k]
        v_late[k - late] = v_ref[k]
        b = starts[k // q4] + k % q4
        insert_row(k_late, v_late, k - late, pos_ref[b] - base, kn_ref[b], vn_ref[b])

    lane_id = lax.broadcasted_iota(jnp.int32, (n_q, 128), 1)
    stats = [jnp.zeros((n_q, 128), jnp.float32)]

    def per_head(tile):
        return jnp.concatenate([jnp.broadcast_to(tile[g:g + 1], (4, head)) for g in range(kv_local)], axis=0)

    def out_at(b, o, m, l):
        k = b - half_seq
        at = starts[2] + k
        s = jnp.sum(q_ref[k] * per_head(kn_ref[at]), axis=1, keepdims=True) * head ** -0.5
        s = jnp.where(core == k // q4, s, NEG)
        top = jnp.maximum(m, s)
        old = jnp.exp(m - top)
        new = jnp.where(core == k // q4, jnp.exp(s - top), 0.0)
        pay_ref[k] = o * old + new.astype(jnp.bfloat16).astype(jnp.float32) * per_head(vn_ref[at])
        stats[0] = put_stats(stats[0], lane_id, k, top, l * old + new)
        if b >= late:
            late_row(b)

    parts = [list(range(half_seq + i, half_seq + i + PART)) for i in range(0, half_seq, PART)]
    attend_parts(parts, lambda i: None, lambda b: q_ref[b - half_seq],
                 lambda b: pos_ref[starts[2] + b - half_seq] - base - 1,
                 k_ref, v_ref, idx_ref, s_ref, out_at)
    pay_ref[half_seq] = stats[0]
    for i in range(EARLY_PARTS):
        for c in write_copies(i, starts, q4, k_ref, v_ref, ko_ref, vo_ref, o_sem):
            c.wait()


def third_kernel(k_late, v_late, k_in, v_in, ko_ref, vo_ref, o_sem):
    n_seq = ko_ref.shape[0]
    starts = quarters(n_seq)
    parts = range(EARLY_PARTS, n_seq // PART)
    for i in parts:
        for c in write_copies(i, starts, n_seq // 4, k_late, v_late, ko_ref, vo_ref, o_sem, EARLY_PARTS):
            c.start()
    for i in parts:
        for c in write_copies(i, starts, n_seq // 4, k_late, v_late, ko_ref, vo_ref, o_sem, EARLY_PARTS):
            c.wait()


def finish_kernel(h_ref, w_ref, mine_ref, sib_ref, got_ref, sib_got_ref, out_ref,
                  w_buf, att, got2, lhs, part, y_in, fin, x_in, d_in, d_in2,
                  w_sem, ys_sem, yr_sem, xs_sem, xr_sem, ds_sem, dr_sem, es_sem, er_sem):
    n_q = mine_ref.shape[1]
    sp = lax.axis_index('sp')
    tp = lax.axis_index('tp')
    x, c = sp // 2, sp % 2
    sib = {'sp': x * 2 + (1 - c)}
    xn = {'sp': (1 - x) * 2 + c}
    yn = {'tp': 1 - tp}

    half_cols = w_buf.shape[1]
    cc = half_cols // OUT_CHUNKS
    q4 = got_ref.shape[0] - 1
    own_col = c * half_cols
    oth_col = (1 - c) * half_cols

    wc = half_cols // DOTS
    per_dot = OUT_CHUNKS // DOTS

    def w_copy(j):
        return pltpu.make_async_copy(
            w_ref.at[:, pl.ds(pl.multiple_of(own_col + j * wc, 128), wc)],
            w_buf.at[:, pl.ds(j * wc, wc)], w_sem.at[j])

    for j in range(DOTS):
        w_copy(j).start()

    barrier = pltpu.get_barrier_semaphore()
    for dev in (sib, xn, yn):
        pl.semaphore_signal(barrier, inc=1, device_id=dev, device_id_type=MESH)

    def remote(src, dst, ssem, rsem, dev):
        return pltpu.make_async_remote_copy(src_ref=src, dst_ref=dst, send_sem=ssem, recv_sem=rsem,
                                            device_id=dev, device_id_type=MESH)

    got2[c] = got_ref[...]
    got2[1 - c] = sib_got_ref[...]

    lane_id = lax.broadcasted_iota(jnp.int32, (n_q, 128), 1)
    far = got2[1, q4]
    far = jnp.where(lane_id % 64 < q4, got2[0, q4], pltpu.roll(far, q4, 1))
    maxes = [mine_ref[2 * q4], sib_ref[2 * q4], far]
    sums = [pltpu.roll(m, 64, 1) for m in maxes]
    top = jnp.maximum(jnp.maximum(maxes[0], maxes[1]), maxes[2])
    factors = [jnp.exp(m - top) for m in maxes]
    inv = 1.0 / (sums[0] * factors[0] + sums[1] * factors[1] + sums[2] * factors[2])
    factors = [f * inv for f in factors]
    for i in range(2 * q4):
        f0, f1, f2 = (jnp.broadcast_to(f[:, i:i + 1], (n_q, 128)) for f in factors)
        att[i] = mine_ref[i] * f0 + sib_ref[i] * f1 + got2[i // q4, i % q4] * f2
    for n in range(n_q):
        lhs[:, n * 128:(n + 1) * 128] = att[:, n, :].astype(jnp.bfloat16)

    y_copy, x_copy, d_copy, e_copy = [], [], [], []
    for t in range(DOTS):
        w_copy(t).wait()
        prod = jnp.dot(lhs[...], w_buf[:, t * wc:(t + 1) * wc], preferred_element_type=jnp.float32)
        if t == 0:
            pl.semaphore_wait(barrier, 3)
        for k in range(per_dot):
            j = t * per_dot + k
            part[j] = prod[:, k * cc:(k + 1) * cc]
            y_copy.append(remote(part.at[j], y_in.at[j], ys_sem.at[j], yr_sem.at[j], yn))
            y_copy[j].start()

    my_rows = pl.ds(pl.multiple_of(x * (2 * q4), 2 * q4), 2 * q4)
    xn_rows = pl.ds(pl.multiple_of((1 - x) * (2 * q4), 2 * q4), 2 * q4)

    def cols(start, j):
        return pl.ds(pl.multiple_of(start + j * cc, 128), cc)

    for j in range(OUT_CHUNKS):
        y_copy[j].wait_recv()
        fin[j] = h_ref[my_rows, cols(own_col, j)].astype(jnp.float32) + (part[j] + y_in[j])
        x_copy.append(remote(fin.at[j], x_in.at[j], xs_sem.at[j], xr_sem.at[j], xn))
        x_copy[j].start()
        d_copy.append(remote(fin.at[j], d_in.at[j], ds_sem.at[j], dr_sem.at[j], sib))
        d_copy[j].start()
        out_ref[my_rows, cols(own_col, j)] = fin[j].astype(jnp.bfloat16)
    for j in range(OUT_CHUNKS):
        x_copy[j].wait_recv()
        e_copy.append(remote(x_in.at[j], d_in2.at[j], es_sem.at[j], er_sem.at[j], sib))
        e_copy[j].start()
        out_ref[xn_rows, cols(own_col, j)] = x_in[j].astype(jnp.bfloat16)
        d_copy[j].wait_recv()
        out_ref[my_rows, cols(oth_col, j)] = d_in[j].astype(jnp.bfloat16)
    for j in range(OUT_CHUNKS):
        e_copy[j].wait_recv()
        out_ref[xn_rows, cols(oth_col, j)] = d_in2[j].astype(jnp.bfloat16)

    for cp in y_copy + x_copy + d_copy + e_copy:
        cp.wait_send()


def solution(mesh):
    cache_spec = P('dp', 'sp', 'tp', None)

    def local_step(hidden, norm_scale, w_qkv, w_out, k_cache, v_cache, positions):
        n_seq, seq_local, kv_local, head = k_cache.shape
        d_model = hidden.shape[1]
        rows = seq_local * kv_local
        n_q = 4 * kv_local
        q4 = n_seq // 4
        vm = pl.BlockSpec(memory_space=pltpu.VMEM)
        hbm = pl.BlockSpec(memory_space=pltpu.HBM)
        dma = pltpu.SemaphoreType.DMA
        f32, bf16 = jnp.float32, jnp.bfloat16
        payload = pltpu.VMEM((q4 + 1, n_q, head), f32)
        payload2 = pltpu.VMEM((2 * q4 + 1, n_q, head), f32)
        k_rows = k_cache.reshape(n_seq, rows, head)
        v_rows = v_cache.reshape(n_seq, rows, head)
        slots = n_seq // PART
        late = pltpu.VMEM((n_seq - EARLY_PARTS * PART, rows, head), bf16)
        w_chunks = len(W_SPLIT)

        def pin(a):
            return pltpu.with_memory_space_constraint(a, pltpu.HBM)

        k_all, v_all, pay, q_own, kn, vn = pl.pallas_call(
            first_kernel,
            out_shape=(pltpu.VMEM((n_seq, rows, head), bf16), pltpu.VMEM((n_seq, rows, head), bf16),
                       payload,
                       pltpu.VMEM((2 * q4, n_q, head), f32), pltpu.VMEM((n_seq, 8, head), f32),
                       pltpu.VMEM((n_seq, 8, head), f32)),
            in_specs=[hbm] * 6,
            out_specs=(vm,) * 6,
            scratch_shapes=[
                pltpu.SMEM((n_seq,), jnp.int32),
                pltpu.VMEM((n_seq, d_model), bf16),
                pltpu.VMEM((d_model // 128, 128), bf16),
                pltpu.VMEM((d_model, 3 * kv_local * head), bf16),
                pltpu.VMEM((n_seq, d_model), bf16),
                pltpu.VMEM((6 * kv_local, n_seq, head), f32),
                pltpu.VMEM((n_seq // 2, n_q, head), f32),
                pltpu.VMEM((n_seq, head), f32),
                pltpu.VMEM((n_q, rows), jnp.int32),
                pltpu.VMEM((2, PART, n_q, rows), f32),
                payload, payload,
                dma((3,)), dma((w_chunks,)), dma((slots,)), dma((slots,)),
                dma((w_chunks + 1,)), dma((w_chunks + 1,)),
            ],
            compiler_params=pltpu.CompilerParams(
                collective_id=1, has_side_effects=True, vmem_limit_bytes=FIRST_VMEM * 1024 * 1024),
            cost_estimate=pl.CostEstimate(flops=2 * 10**10, bytes_accessed=4 * 10**7, transcendentals=0),
            name='first',
        )(*map(pin, (positions, hidden, norm_scale.reshape(d_model // 128, 128), w_qkv, k_rows, v_rows)))

        got = lax.ppermute(pay, 'sp', [(i, i ^ 2) for i in range(4)])

        k_part, v_part, mine, k_late, v_late = pl.pallas_call(
            second_kernel,
            out_shape=(jax.ShapeDtypeStruct((n_seq, rows, head), bf16),
                       jax.ShapeDtypeStruct((n_seq, rows, head), bf16), payload2, late, late),
            in_specs=[hbm, vm, vm, vm, vm, vm],
            out_specs=(hbm, hbm, vm, vm, vm),
            scratch_shapes=[
                pltpu.SMEM((n_seq,), jnp.int32),
                pltpu.VMEM((n_q, rows), jnp.int32),
                pltpu.VMEM((2, PART, n_q, rows), f32),
                dma((1,)), dma((2, n_seq // PART)),
            ],
            compiler_params=pltpu.CompilerParams(vmem_limit_bytes=12 * 1024 * 1024),
            cost_estimate=pl.CostEstimate(flops=2 * 10**10, bytes_accessed=4 * 10**7, transcendentals=0),
            name='second',
        )(positions, q_own, kn, vn, k_all, v_all)

        swap = [(i, i ^ 1) for i in range(4)]
        sib_mine = lax.ppermute(mine, 'sp', swap)
        sib_got = lax.ppermute(got, 'sp', swap)

        k_upd, v_upd = pl.pallas_call(
            third_kernel,
            out_shape=(jax.ShapeDtypeStruct((n_seq, rows, head), bf16),
                       jax.ShapeDtypeStruct((n_seq, rows, head), bf16)),
            in_specs=[vm, vm, hbm, hbm],
            out_specs=(hbm, hbm),
            input_output_aliases={2: 0, 3: 1},
            scratch_shapes=[dma((2, n_seq // PART))],
            compiler_params=pltpu.CompilerParams(vmem_limit_bytes=12 * 1024 * 1024),
            cost_estimate=pl.CostEstimate(flops=2 * 10**10, bytes_accessed=4 * 10**7, transcendentals=0),
            name='third',
        )(k_late, v_late, k_part, v_part)

        half_cols = d_model // 2
        cc = half_cols // OUT_CHUNKS
        chunk = pltpu.VMEM((OUT_CHUNKS, 2 * q4, cc), f32)
        h_out = pl.pallas_call(
            finish_kernel,
            out_shape=jax.ShapeDtypeStruct((n_seq, d_model), bf16),
            in_specs=[vm, hbm, vm, vm, vm, vm],
            out_specs=vm,
            scratch_shapes=[
                pltpu.VMEM((w_out.shape[0], half_cols), bf16),
                pltpu.VMEM((2 * q4, n_q, head), f32),
                pltpu.VMEM((2, q4 + 1, n_q, head), f32),
                pltpu.VMEM((2 * q4, n_q * head), bf16),
                chunk, chunk, chunk, chunk, chunk, chunk,
                dma((DOTS,)),
                dma((OUT_CHUNKS,)), dma((OUT_CHUNKS,)),
                dma((OUT_CHUNKS,)), dma((OUT_CHUNKS,)),
                dma((OUT_CHUNKS,)), dma((OUT_CHUNKS,)),
                dma((OUT_CHUNKS,)), dma((OUT_CHUNKS,)),
            ],
            compiler_params=pltpu.CompilerParams(
                collective_id=0, has_side_effects=True, vmem_limit_bytes=50 * 1024 * 1024),
            name='finish',
        )(hidden, pin(w_out), mine, sib_mine, got, sib_got)
        return h_out, k_upd.reshape(k_cache.shape), v_upd.reshape(v_cache.shape)

    return jax.shard_map(
        local_step,
        mesh=mesh,
        in_specs=(P('dp', None), P(None), P(None, 'tp'), P('tp', None), cache_spec, cache_spec, P('dp')),
        out_specs=(P('dp', None), cache_spec, cache_spec),
        check_vma=False,
    )
```
